8 devices in a mesh: fsdp: 8 (over z, y, x, core).
Axes of the slice: x: 2, y: 2, z: 1, core: 2. Of those that a mesh axis runs over, the one named last changes fastest.
Arguments:
- x: bfloat16 [64, 384, 512], P('fsdp')
- lengths: int32 [64], P('fsdp')
- d_y: bfloat16 [64, 384, 512], P('fsdp')
- w_attn: bfloat16 [2, 4, 512, 512], P(None, None, 'fsdp')
- b_attn: bfloat16 [2, 4, 512], P(None, None, 'fsdp')
- ln_par: bfloat16 [2, 4, 512], P(None, None, 'fsdp')
- w_up: bfloat16 [2, 512, 2048], P(None, 'fsdp')
- b_up: bfloat16 [2, 2048], P(None, 'fsdp')
- w_down: bfloat16 [2, 2048, 512], P(None, 'fsdp')
- b_down: bfloat16 [2, 512], P(None, 'fsdp')
Outputs:
- output 1: bfloat16 [64, 384, 512], P('fsdp')
- output 2: float32 [2, 4, 512, 512], P(None, None, 'fsdp')
- output 3: float32 [2, 4, 512], P(None, None, 'fsdp')
- output 4: float32 [2, 4, 512], P(None, None, 'fsdp')
- output 5: float32 [2, 512, 2048], P(None, 'fsdp')
- output 6: float32 [2, 2048], P(None, 'fsdp')
- output 7: float32 [2, 2048, 512], P(None, 'fsdp')
- output 8: float32 [2, 512], P(None, 'fsdp')
All inputs are finite; a program needn't handle non-finite values.
Results may differ from the reference program's by a relative error of at most 0.0135649.
Values are sent between devices in bfloat16 or wider.
A program may use at most 1 GiB of HBM per device.

```python
import jax
import jax.numpy as jnp
from jax import lax

MODEL_DIM = 512
FFN_DIM = 2048
HEAD_DIM = 64
NUM_LAYERS = 2
SEQ_LEN = 384
SEQ_DEV = 8
GROUP_SIZE = 8
EPS = 1e-5
THETA = 10000.0
NUM_HEADS = MODEL_DIM // HEAD_DIM
BATCH = SEQ_DEV * GROUP_SIZE
MIN_LEN = SEQ_LEN // 8


def setup_inputs(seed: int = 0) -> dict:
    key_list = jax.random.split(jax.random.key(seed), 10)
    seq_index = jnp.arange(BATCH)
    drawn_len = jax.random.randint(key_list[1], (BATCH,), MIN_LEN, SEQ_LEN + 1)
    lengths = jnp.where(seq_index == 0, SEQ_LEN, jnp.where(seq_index == 1, MIN_LEN, drawn_len)).astype(jnp.int32)
    act_shape = (BATCH, SEQ_LEN, MODEL_DIM)
    dy_scale = float(BATCH * SEQ_LEN) ** -0.25
    ln_base = jnp.array([1.0, 0.0, 1.0, 0.0], dtype=jnp.float32)[None, :, None]
    return {
        'x': jax.random.normal(key_list[0], act_shape, jnp.float32).astype(jnp.bfloat16),
        'lengths': lengths,
        'd_y': (dy_scale * jax.random.normal(key_list[2], act_shape, jnp.float32)).astype(jnp.bfloat16),
        'w_attn': (MODEL_DIM ** -0.5 * jax.random.normal(key_list[3], (NUM_LAYERS, 4, MODEL_DIM, MODEL_DIM), jnp.float32)).astype(jnp.bfloat16),
        'b_attn': (0.3 * jax.random.normal(key_list[4], (NUM_LAYERS, 4, MODEL_DIM), jnp.float32)).astype(jnp.bfloat16),
        'ln_par': (ln_base + 0.2 * jax.random.normal(key_list[5], (NUM_LAYERS, 4, MODEL_DIM), jnp.float32)).astype(jnp.bfloat16),
        'w_up': (MODEL_DIM ** -0.5 * jax.random.normal(key_list[6], (NUM_LAYERS, MODEL_DIM, FFN_DIM), jnp.float32)).astype(jnp.bfloat16),
        'b_up': (0.5 * jax.random.normal(key_list[7], (NUM_LAYERS, FFN_DIM), jnp.float32)).astype(jnp.bfloat16),
        'w_down': (FFN_DIM ** -0.5 * jax.random.normal(key_list[8], (NUM_LAYERS, FFN_DIM, MODEL_DIM), jnp.float32)).astype(jnp.bfloat16),
        'b_down': (0.3 * jax.random.normal(key_list[9], (NUM_LAYERS, MODEL_DIM), jnp.float32)).astype(jnp.bfloat16),
    }


def to_bf16(tensor):
    return tensor.astype(jnp.bfloat16).astype(jnp.float32)


def norm_fwd(x_in, gain, shift):
    row_mean = jnp.mean(x_in, axis=-1, keepdims=True)
    centered = x_in - row_mean
    variance = jnp.mean(centered * centered, axis=-1, keepdims=True)
    return centered * lax.rsqrt(variance + EPS) * gain + shift


def rotary_tables():
    half_dim = HEAD_DIM // 2
    inv_freq = 1.0 / (THETA ** (jnp.arange(half_dim, dtype=jnp.float32) * (2.0 / HEAD_DIM)))
    angles = jnp.arange(SEQ_LEN, dtype=jnp.float32)[:, None] * inv_freq[None, :]
    return jnp.cos(angles)[:, None, :], jnp.sin(angles)[:, None, :]


def rotate(tensor, cos_tab, sin_tab):
    half_dim = HEAD_DIM // 2
    first_half = tensor[..., :half_dim]
    second_half = tensor[..., half_dim:]
    return jnp.concatenate([first_half * cos_tab - second_half * sin_tab, second_half * cos_tab + first_half * sin_tab], axis=-1)


def layer_fwd(x, weights, lengths, tables):
    w_attn, b_attn, ln_par, w_up, b_up, w_down, b_down = weights
    cos_tab, sin_tab = tables
    num_seq = x.shape[0]
    h_one = to_bf16(norm_fwd(x, ln_par[0], ln_par[1]))
    projected = jnp.einsum('bld,kde->kble', h_one, w_attn[:3]) + b_attn[:3, None, None, :]
    projected = projected.reshape(3, num_seq, SEQ_LEN, NUM_HEADS, HEAD_DIM)
    query_rot = to_bf16(rotate(projected[0] * (HEAD_DIM ** -0.5), cos_tab, sin_tab))
    key_rot = to_bf16(rotate(projected[1], cos_tab, sin_tab))
    values = to_bf16(projected[2])
    scores = jnp.einsum('bqhd,bkhd->bhqk', query_rot, key_rot)
    key_valid = jnp.arange(SEQ_LEN)[None, None, None, :] < lengths[:, None, None, None]
    attn_probs = to_bf16(jax.nn.softmax(jnp.where(key_valid, scores, -1e30), axis=-1))
    context = to_bf16(jnp.einsum('bhqk,bkhd->bqhd', attn_probs, values)).reshape(num_seq, SEQ_LEN, MODEL_DIM)
    x_mid = to_bf16(x + jnp.einsum('bld,de->ble', context, w_attn[3]) + b_attn[3])
    h_two = to_bf16(norm_fwd(x_mid, ln_par[2], ln_par[3]))
    act_out = to_bf16(jax.nn.gelu(jnp.einsum('bld,df->blf', h_two, w_up) + b_up, approximate=False))
    return to_bf16(x_mid + jnp.einsum('blf,fd->bld', act_out, w_down) + b_down)


def reference(x, lengths, d_y, w_attn, b_attn, ln_par, w_up, b_up, w_down, b_down):
    params = tuple(tensor.astype(jnp.float32) for tensor in (w_attn, b_attn, ln_par, w_up, b_up, w_down, b_down))
    tables = rotary_tables()

    def stack_fwd(x_block, param_set, len_block):
        hidden = x_block
        for layer_idx in range(NUM_LAYERS):
            hidden = layer_fwd(hidden, tuple(tensor[layer_idx] for tensor in param_set), len_block, tables)
        return hidden

    def block_step(grad_acc, block_in):
        x_block, len_block, dy_block = block_in

        def block_fwd(x_local, param_local):
            return stack_fwd(x_local, param_local, len_block)

        _, pull_back = jax.vjp(block_fwd, x_block.astype(jnp.float32), params)
        d_x_block, d_params = pull_back(dy_block.astype(jnp.float32))
        return jax.tree.map(jnp.add, grad_acc, d_params), d_x_block.astype(jnp.bfloat16)

    grad_zero = jax.tree.map(jnp.zeros_like, params)
    blocks_in = (x.reshape(GROUP_SIZE, SEQ_DEV, SEQ_LEN, MODEL_DIM), lengths.reshape(GROUP_SIZE, SEQ_DEV), d_y.reshape(GROUP_SIZE, SEQ_DEV, SEQ_LEN, MODEL_DIM))
    grad_sum, d_x = lax.scan(block_step, grad_zero, blocks_in)
    return (d_x.reshape(BATCH, SEQ_LEN, MODEL_DIM), grad_sum[0], grad_sum[1], grad_sum[2], grad_sum[3], grad_sum[4], grad_sum[5], grad_sum[6])
```

```python
import math
import jax
import jax.numpy as jnp
from jax import lax
from jax.experimental import pallas as pl
from jax.experimental.pallas import tpu as pltpu
from jax.sharding import PartitionSpec as P

HEAD_DIM = 64
EPS = 1e-5
THETA = 10000.0
NEG_BIG = -1e30
BF16 = jnp.bfloat16
F32 = jnp.float32
VMEM_BYTES = 60 * 1024 * 1024
GROUP = 256
HEADS_GROUP = 4
KEY_BLOCK = 128

NN = (((1,), (0,)), ((), ()))
NT = (((1,), (1,)), ((), ()))
TN = (((0,), (0,)), ((), ()))


def mm(a, b, dims=NN):
    return lax.dot_general(a, b, dims, preferred_element_type=F32)


def rotary_tables(seq_len):
    half_dim = HEAD_DIM // 2
    inv_freq = 1.0 / (THETA ** (jnp.arange(half_dim, dtype=F32) * (2.0 / HEAD_DIM)))
    angles = jnp.arange(seq_len, dtype=F32)[:, None] * inv_freq[None, :]
    return jnp.tile(jnp.cos(angles), (1, HEADS_GROUP)), jnp.tile(jnp.sin(angles), (1, HEADS_GROUP))


def normalize(x_f32):
    centered = x_f32 - jnp.mean(x_f32, axis=-1, keepdims=True)
    rstd = lax.rsqrt(jnp.mean(centered * centered, axis=-1, keepdims=True) + EPS)
    return centered * rstd, rstd


def norm_bwd(d_h, x_hat, rstd, gain):
    d_hat = d_h * gain
    mean_d = jnp.mean(d_hat, axis=-1, keepdims=True)
    mean_dx = jnp.mean(d_hat * x_hat, axis=-1, keepdims=True)
    return rstd * (d_hat - mean_d - x_hat * mean_dx)


def rot_halves(first, second, cos_tab, sin_tab):
    return first * cos_tab - second * sin_tab, second * cos_tab + first * sin_tab


def unrot_halves(first, second, cos_tab, sin_tab):
    return first * cos_tab + second * sin_tab, second * cos_tab - first * sin_tab


def head_masks():
    lane = lax.broadcasted_iota(jnp.int32, (1, GROUP), 1)
    qk = [((lane % 128) // 32 == h).astype(F32).astype(BF16) for h in range(HEADS_GROUP)]
    vo = [(lane // 64 == h).astype(F32).astype(BF16) for h in range(HEADS_GROUP)]
    return qk, vo


def stack_masked(block, masks):
    return jnp.concatenate([block * m for m in masks], axis=0)


def for_key_width(length, seq_len, body):
    blocks = (length + KEY_BLOCK - 1) // KEY_BLOCK
    for n in range(1, seq_len // KEY_BLOCK + 1):
        @pl.when(blocks == n)
        def _(n=n):
            body(n * KEY_BLOCK)


def attn_fwd_kernel(len_ref, x_ref, w_ref, vec_ref, cos_ref, sin_ref, q_ref, k_ref, v_ref, p_ref, ctx_ref, mid_ref):
    seq_len, model = x_ref.shape[1:]
    length = len_ref[pl.program_id(0)]
    x_hat, _ = normalize(x_ref[0].astype(F32))
    h_one = (x_hat * vec_ref[4:5, :] + vec_ref[5:6, :]).astype(BF16)
    cos_tab, sin_tab = cos_ref[...], sin_ref[...]
    for i, out in enumerate((q_ref, k_ref)):
        proj = mm(h_one, w_ref[:, i * 64:(i + 1) * 64, :].reshape(model, model)) + vec_ref[i:i + 1, :]
        if i == 0:
            proj = proj * (HEAD_DIM ** -0.5)
        for g in range(model // GROUP):
            lo = g * GROUP
            first, second = rot_halves(proj[:, lo:lo + 128], proj[:, lo + 128:lo + 256], cos_tab, sin_tab)
            out[0, :, lo:lo + 128] = first.astype(BF16)
            out[0, :, lo + 128:lo + 256] = second.astype(BF16)
    proj = mm(h_one, w_ref[:, 128:192, :].reshape(model, model)) + vec_ref[2:3, :]
    v_ref[0] = proj.astype(BF16)
    qk_masks, vo_masks = head_masks()

    def attend(width):
        valid = lax.broadcasted_iota(jnp.int32, (1, width), 1) < length
        for g in range(model // GROUP):
            lo = g * GROUP
            k_cat = stack_masked(k_ref[0, 0:width, lo:lo + GROUP], qk_masks)
            scores = mm(q_ref[0, :, lo:lo + GROUP], k_cat, NT)
            probs = []
            for h in range(HEADS_GROUP):
                s_h = jnp.where(valid, scores[:, h * width:(h + 1) * width], NEG_BIG)
                e_h = jnp.exp(s_h - jnp.max(s_h, axis=-1, keepdims=True))
                p_h = (e_h * (1.0 / jnp.sum(e_h, axis=-1, keepdims=True))).astype(BF16)
                base = (g * HEADS_GROUP + h) * seq_len
                p_ref[0, :, base:base + width] = p_h
                probs.append(p_h)
            v_cat = stack_masked(v_ref[0, 0:width, lo:lo + GROUP], vo_masks)
            ctx_ref[0, :, lo:lo + GROUP] = mm(jnp.concatenate(probs, axis=1), v_cat).astype(BF16)

    for_key_width(length, seq_len, attend)
    attn_out = mm(ctx_ref[0], w_ref[:, 192:256, :].reshape(model, model))
    mid_ref[0] = (x_ref[0].astype(F32) + attn_out + vec_ref[3:4, :]).astype(BF16)


def mlp_fwd_kernel(mid_ref, w_ref, vec_ref, y_ref, act_ref, slope_ref):
    model = mid_ref.shape[1]
    mid = mid_ref[...].astype(F32)
    x_hat, _ = normalize(mid)
    h_two = (x_hat * vec_ref[6:7, :] + vec_ref[7:8, :]).astype(BF16)
    for c in range(4):
        cols = slice(c * model, (c + 1) * model)
        pre = mm(h_two, w_ref[:, c * 64:(c + 1) * 64, :].reshape(model, model)) + vec_ref[9 + c:10 + c, :]
        cdf = 0.5 * lax.erf(pre * (1.0 / math.sqrt(2.0))) + 0.5
        density = jnp.exp(pre * pre * -0.5) * (1.0 / math.sqrt(2.0 * math.pi))
        act_ref[:, cols] = (pre * cdf).astype(BF16)
        slope_ref[:, cols] = cdf + pre * density
    out = mm(act_ref[...], w_ref[:, 256:512, :].reshape(4 * model, model))
    y_ref[...] = (mid + out + vec_ref[8:9, :]).astype(BF16)


def mlp_bwd_kernel(dout_ref, mid_ref, act_ref, slope_ref, w_ref, vec_ref, dmid_ref, gw_ref, gs_ref, dpre_ref):
    model = mid_ref.shape[1]

    @pl.when(pl.program_id(0) == 0)
    def _():
        gw_ref[...] = jnp.zeros_like(gw_ref)
        gs_ref[...] = jnp.zeros_like(gs_ref)

    x_hat, rstd = normalize(mid_ref[...].astype(F32))
    h_two = (x_hat * vec_ref[6:7, :] + vec_ref[7:8, :]).astype(BF16)
    d_out = dout_ref[...]
    d_h = None
    for c in range(4):
        cols = slice(c * model, (c + 1) * model)
        d_act = mm(d_out, w_ref[2 * c:2 * c + 2, 256:512, :].reshape(model, model), NT)
        d_pre = d_act * slope_ref[:, cols]
        gs_ref[c:c + 1, :] += jnp.sum(d_pre, axis=0, keepdims=True)
        dpre_ref[:, cols] = d_pre.astype(BF16)
    for c in range(4):
        cols = slice(c * model, (c + 1) * model)
        gw_ref[2 * c:2 * c + 2, 256:512, :] += mm(act_ref[:, cols], d_out, TN).reshape(2, 256, model)
        gw_ref[:, c * 64:(c + 1) * 64, :] += mm(h_two, dpre_ref[:, cols], TN).reshape(8, 64, model)
        part = mm(dpre_ref[:, cols], w_ref[:, c * 64:(c + 1) * 64, :].reshape(model, model), NT)
        d_h = part if d_h is None else d_h + part
    d_out_f32 = d_out.astype(F32)
    gs_ref[4:5, :] += jnp.sum(d_out_f32, axis=0, keepdims=True)
    gs_ref[5:6, :] += jnp.sum(d_h * x_hat, axis=0, keepdims=True)
    gs_ref[6:7, :] += jnp.sum(d_h, axis=0, keepdims=True)
    dmid_ref[...] = (d_out_f32 + norm_bwd(d_h, x_hat, rstd, vec_ref[6:7, :])).astype(BF16)


def attn_bwd_kernel(len_ref, dmid_ref, x_ref, q_ref, k_ref, v_ref, p_ref, ctx_ref, w_ref, vec_ref, cos_ref, sin_ref,
                    dx_ref, gw_ref, gs_ref, dctx_ref, dq_ref, dk_ref, dv_ref):
    seq_len, model = x_ref.shape[1:]
    length = len_ref[pl.program_id(0)]

    @pl.when(pl.program_id(0) == 0)
    def _():
        gw_ref[...] = jnp.zeros_like(gw_ref)
        gs_ref[...] = jnp.zeros_like(gs_ref)

    d_mid = dmid_ref[0]
    d_mid_f32 = d_mid.astype(F32)
    gs_ref[3:4, :] += jnp.sum(d_mid_f32, axis=0, keepdims=True)
    gw_ref[:, 192:256, :] += mm(ctx_ref[0], d_mid, TN).reshape(8, 64, model)
    dctx_ref[...] = mm(d_mid, w_ref[:, 192:256, :].reshape(model, model), NT).astype(BF16)
    qk_masks, vo_masks = head_masks()

    def attend(width):
        for g in range(model // GROUP):
            lo = g * GROUP
            d_ctx = dctx_ref[:, lo:lo + GROUP]
            d_probs = mm(d_ctx, stack_masked(v_ref[0, 0:width, lo:lo + GROUP], vo_masks), NT)
            ds_list, dst_list, pt_list = [], [], []
            for h in range(HEADS_GROUP):
                base = (g * HEADS_GROUP + h) * seq_len
                p_bf = p_ref[0, :, base:base + width]
                p_h = p_bf.astype(F32)
                dp_h = d_probs[:, h * width:(h + 1) * width]
                ds_h = (p_h * (dp_h - jnp.sum(dp_h * p_h, axis=-1, keepdims=True))).astype(BF16)
                ds_list.append(ds_h)
                dst_list.append(ds_h.T)
                pt_list.append(p_bf.T)
            k_cat = stack_masked(k_ref[0, 0:width, lo:lo + GROUP], qk_masks)
            dq_ref[:, lo:lo + GROUP] = mm(jnp.concatenate(ds_list, axis=1), k_cat)
            q_cat = stack_masked(q_ref[0, :, lo:lo + GROUP], qk_masks)
            dk_ref[0:width, lo:lo + GROUP] = mm(jnp.concatenate(dst_list, axis=1), q_cat)
            do_cat = stack_masked(d_ctx, vo_masks)
            dv_ref[0:width, lo:lo + GROUP] = mm(jnp.concatenate(pt_list, axis=1), do_cat)
        if width < seq_len:
            dk_ref[width:, :] = jnp.zeros((seq_len - width, model), F32)
            dv_ref[width:, :] = jnp.zeros((seq_len - width, model), F32)

    for_key_width(length, seq_len, attend)
    cos_tab, sin_tab = cos_ref[...], sin_ref[...]
    x_hat, rstd = normalize(x_ref[0].astype(F32))
    h_one = (x_hat * vec_ref[4:5, :] + vec_ref[5:6, :]).astype(BF16)
    d_h = None
    for i, src in enumerate((dq_ref, dk_ref, dv_ref)):
        if i < 2:
            pieces = []
            for g in range(model // GROUP):
                lo = g * GROUP
                pieces.extend(unrot_halves(src[:, lo:lo + 128], src[:, lo + 128:lo + 256], cos_tab, sin_tab))
            d_proj = jnp.concatenate(pieces, axis=1)
            if i == 0:
                d_proj = d_proj * (HEAD_DIM ** -0.5)
        else:
            d_proj = src[...]
        d_proj = d_proj.astype(BF16)
        gs_ref[i:i + 1, :] += jnp.sum(d_proj.astype(F32), axis=0, keepdims=True)
        gw_ref[:, i * 64:(i + 1) * 64, :] += mm(h_one, d_proj, TN).reshape(8, 64, model)
        part = mm(d_proj, w_ref[:, i * 64:(i + 1) * 64, :].reshape(model, model), NT)
        d_h = part if d_h is None else d_h + part
    gs_ref[4:5, :] += jnp.sum(d_h * x_hat, axis=0, keepdims=True)
    gs_ref[5:6, :] += jnp.sum(d_h, axis=0, keepdims=True)
    dx_ref[0] = (d_mid_f32 + norm_bwd(d_h, x_hat, rstd, vec_ref[4:5, :])).astype(BF16)


def seq_spec(*tail):
    return pl.BlockSpec((1,) + tail, lambda b, *_: (b,) + (0,) * len(tail))


def row_spec(rows, cols):
    return pl.BlockSpec((rows, cols), lambda b, *_: (b, 0))


def whole(shape):
    return pl.BlockSpec(shape, lambda *_: (0,) * len(shape))


def params():
    return pltpu.CompilerParams(dimension_semantics=('arbitrary',), vmem_limit_bytes=VMEM_BYTES)


def cost(flops, nbytes):
    return pl.CostEstimate(flops=int(flops), bytes_accessed=int(nbytes), transcendentals=0)


def sds(shape, dtype):
    return jax.ShapeDtypeStruct(shape, dtype)


def attn_forward(lengths, x, w, vec, tables):
    n, seq_len, model = x.shape
    heads = model // HEAD_DIM
    act = sds(x.shape, BF16)
    spec = seq_spec(seq_len, model)
    return pl.pallas_call(
        attn_fwd_kernel,
        grid_spec=pltpu.PrefetchScalarGridSpec(
            num_scalar_prefetch=1, grid=(n,),
            in_specs=[spec, whole(w.shape), whole(vec.shape), whole(tables[0].shape), whole(tables[1].shape)],
            out_specs=[spec, spec, spec, seq_spec(seq_len, heads * seq_len), spec, spec]),
        out_shape=[act, act, act, sds((n, seq_len, heads * seq_len), BF16), act, act],
        compiler_params=params(), cost_estimate=cost(16e9, 40e6), name='attn_fwd',
    )(lengths, x, w, vec, *tables)


def mlp_forward(mid, w, vec, rows):
    tokens, model = mid.shape
    return pl.pallas_call(
        mlp_fwd_kernel, grid=(tokens // rows,),
        in_specs=[row_spec(rows, model), whole(w.shape), whole(vec.shape)],
        out_specs=[row_spec(rows, model), row_spec(rows, 4 * model), row_spec(rows, 4 * model)],
        out_shape=[sds(mid.shape, BF16), sds((tokens, 4 * model), BF16), sds((tokens, 4 * model), F32)],
        compiler_params=params(), cost_estimate=cost(13e9, 50e6), name='mlp_fwd',
    )(mid, w, vec)


def mlp_backward(d_out, mid, act, slope, w, vec, rows):
    tokens, model = mid.shape
    wide = row_spec(rows, 4 * model)
    return pl.pallas_call(
        mlp_bwd_kernel, grid=(tokens // rows,),
        in_specs=[row_spec(rows, model), row_spec(rows, model), wide, wide, whole(w.shape), whole(vec.shape)],
        out_specs=[row_spec(rows, model), whole(w.shape), whole((8, model))],
        out_shape=[sds(mid.shape, BF16), sds(w.shape, F32), sds((8, model), F32)],
        scratch_shapes=[pltpu.VMEM((rows, 4 * model), BF16)],
        compiler_params=params(), cost_estimate=cost(26e9, 60e6), name='mlp_bwd',
    )(d_out, mid, act, slope, w, vec)


def attn_backward(lengths, d_mid, x, saved, w, vec, tables):
    n, seq_len, model = x.shape
    heads = model // HEAD_DIM
    spec = seq_spec(seq_len, model)
    return pl.pallas_call(
        attn_bwd_kernel,
        grid_spec=pltpu.PrefetchScalarGridSpec(
            num_scalar_prefetch=1, grid=(n,),
            in_specs=[spec, spec, spec, spec, spec, seq_spec(seq_len, heads * seq_len), spec, whole(w.shape),
                      whole(vec.shape), whole(tables[0].shape), whole(tables[1].shape)],
            out_specs=[spec, whole(w.shape), whole((8, model))],
            scratch_shapes=[pltpu.VMEM((seq_len, model), BF16)] + [pltpu.VMEM((seq_len, model), F32)] * 3),
        out_shape=[sds(x.shape, BF16), sds(w.shape, F32), sds((8, model), F32)],
        compiler_params=params(), cost_estimate=cost(30e9, 50e6), name='attn_bwd',
    )(lengths, d_mid, x, *saved, w, vec, *tables)


def permute_cols(arr):
    lead = arr.shape[:-1]
    return arr.reshape(lead + (-1, HEADS_GROUP, 2, 32)).swapaxes(-3, -2).reshape(arr.shape)


def unpermute_cols(arr):
    lead = arr.shape[:-1]
    return arr.reshape(lead + (-1, 2, HEADS_GROUP, 32)).swapaxes(-3, -2).reshape(arr.shape)


def solution(mesh):
    axis = mesh.axis_names[0]
    batch_spec = P(axis)
    weight_specs = (P(None, None, axis, None), P(None, None, axis), P(None, None, axis),
                    P(None, axis, None), P(None, axis), P(None, axis, None), P(None, axis))

    def device_step(x, lengths, d_y, w_attn, b_attn, ln_par, w_up, b_up, w_down, b_down):
        n_layers, _, part, model = w_attn.shape
        n_seq, seq_len = x.shape[:2]
        tables = rotary_tables(seq_len)
        rows = 384

        def gather(a):
            return lax.all_gather(a, axis, axis=0, tiled=False)

        small = jnp.concatenate([b_attn, ln_par, b_down[:, None, :], b_up.reshape(n_layers, 4, part)], axis=1)
        small_all = gather(small)
        vecs = []
        for l in range(n_layers):
            s = small_all[:, l]
            nine = s[:, :9].swapaxes(0, 1).reshape(9, model)
            nine = jnp.concatenate([permute_cols(nine[:2]), nine[2:]], axis=0)
            up = s[:, 9:].reshape(4, model)
            vecs.append(jnp.concatenate([nine, up, jnp.zeros((3, model), BF16)], axis=0).astype(F32))
        attn_w, mlp_w = [], []
        for l in range(n_layers):
            qk = permute_cols(w_attn[l, :2])
            attn_w.append(gather(jnp.concatenate([qk, w_attn[l, 2:]], axis=0).reshape(4 * part, model)))
            up = w_up[l].reshape(part, 4, model).swapaxes(0, 1).reshape(4 * part, model)
            mlp_w.append(gather(jnp.concatenate([up, w_down[l]], axis=0)))

        hidden = x
        saved = []
        for l in range(n_layers):
            q, k, v, probs, ctx, mid = attn_forward(lengths, hidden, attn_w[l], vecs[l], tables)
            mid2 = mid.reshape(n_seq * seq_len, model)
            y, act, slope = mlp_forward(mid2, mlp_w[l], vecs[l], rows)
            saved.append((hidden, (q, k, v, probs, ctx), mid2, act, slope))
            hidden = y.reshape(x.shape)

        grad = d_y.reshape(n_seq * seq_len, model)
        g_attn, g_mlp, g_small = [None] * n_layers, [None] * n_layers, [None] * n_layers
        for l in reversed(range(n_layers)):
            x_in, attn_saved, mid2, act, slope = saved[l]
            d_mid, gw_mlp, gs_mlp = mlp_backward(grad, mid2, act, slope, mlp_w[l], vecs[l], rows)
            g_mlp[l] = lax.psum_scatter(gw_mlp, axis, scatter_dimension=0, tiled=False)
            d_x, gw_attn, gs_attn = attn_backward(lengths, d_mid.reshape(x.shape), x_in, attn_saved, attn_w[l], vecs[l], tables)
            g_attn[l] = lax.psum_scatter(gw_attn, axis, scatter_dimension=0, tiled=False)
            grad = d_x.reshape(n_seq * seq_len, model)
            gqk = unpermute_cols(gs_attn[:2])
            nine = jnp.concatenate([gqk, gs_attn[2:6], gs_mlp[5:7], gs_mlp[4:5]], axis=0)
            nine = nine.reshape(9, 8, part).swapaxes(0, 1)
            g_small[l] = jnp.concatenate([nine, gs_mlp[:4].reshape(8, 4, part)], axis=1)
        small_sum = lax.psum_scatter(jnp.stack(g_small, axis=1), axis, scatter_dimension=0, tiled=False)

        g_a = jnp.stack(g_attn).reshape(n_layers, 4, part, model)
        g_a = jnp.concatenate([unpermute_cols(g_a[:, :2]), g_a[:, 2:]], axis=1)
        g_m = jnp.stack(g_mlp)
        g_up = g_m[:, :4 * part].reshape(n_layers, 4, part, model).swapaxes(1, 2).reshape(n_layers, part, 4 * model)
        g_down = g_m[:, 4 * part:]
        return (grad.reshape(x.shape), g_a, small_sum[:, 0:4], small_sum[:, 4:8], g_up,
                small_sum[:, 9:13].reshape(n_layers, 4 * part), g_down, small_sum[:, 8])

    return jax.shard_map(device_step, mesh=mesh,
                         in_specs=(batch_spec, batch_spec, batch_spec) + weight_specs,
                         out_specs=(batch_spec,) + weight_specs,
                         check_vma=False)
```

```python
import math
import jax
import jax.numpy as jnp
from jax import lax
from jax.experimental import pallas as pl
from jax.experimental.pallas import tpu as pltpu
from jax.sharding import PartitionSpec as P

HEAD_DIM = 64
EPS = 1e-5
THETA = 10000.0
NEG_BIG = -1e30
BF16 = jnp.bfloat16
F32 = jnp.float32
VMEM_BYTES = 60 * 1024 * 1024
GROUP = 256
HEADS_GROUP = 4
KEY_BLOCK = 128

NN = (((1,), (0,)), ((), ()))
NT = (((1,), (1,)), ((), ()))
TN = (((0,), (0,)), ((), ()))


def mm(a, b, dims=NN):
    return lax.dot_general(a, b, dims, preferred_element_type=F32)


def rotary_tables(seq_len):
    half_dim = HEAD_DIM // 2
    inv_freq = 1.0 / (THETA ** (jnp.arange(half_dim, dtype=F32) * (2.0 / HEAD_DIM)))
    angles = jnp.arange(seq_len, dtype=F32)[:, None] * inv_freq[None, :]
    return jnp.tile(jnp.cos(angles), (1, HEADS_GROUP)), jnp.tile(jnp.sin(angles), (1, HEADS_GROUP))


def normalize(x_f32):
    centered = x_f32 - jnp.mean(x_f32, axis=-1, keepdims=True)
    rstd = lax.rsqrt(jnp.mean(centered * centered, axis=-1, keepdims=True) + EPS)
    return centered * rstd, rstd


def norm_bwd(d_h, x_hat, rstd, gain):
    d_hat = d_h * gain
    mean_d = jnp.mean(d_hat, axis=-1, keepdims=True)
    mean_dx = jnp.mean(d_hat * x_hat, axis=-1, keepdims=True)
    return rstd * (d_hat - mean_d - x_hat * mean_dx)


def rot_halves(first, second, cos_tab, sin_tab):
    return first * cos_tab - second * sin_tab, second * cos_tab + first * sin_tab


def unrot_halves(first, second, cos_tab, sin_tab):
    return first * cos_tab + second * sin_tab, second * cos_tab - first * sin_tab


def head_masks():
    lane = lax.broadcasted_iota(jnp.int32, (1, GROUP), 1)
    qk = [((lane % 128) // 32 == h).astype(F32).astype(BF16) for h in range(HEADS_GROUP)]
    vo = [(lane // 64 == h).astype(F32).astype(BF16) for h in range(HEADS_GROUP)]
    return qk, vo


def stack_masked(block, masks):
    return jnp.concatenate([block * m for m in masks], axis=0)


def for_key_width(length, seq_len, body):
    blocks = (length + KEY_BLOCK - 1) // KEY_BLOCK
    for n in range(1, seq_len // KEY_BLOCK + 1):
        @pl.when(blocks == n)
        def _(n=n):
            body(n * KEY_BLOCK)


def attn_fwd_kernel(len_ref, x_ref, w_ref, vec_ref, cos_ref, sin_ref, q_ref, k_ref, v_ref, p_ref, ctx_ref, mid_ref):
    seq_len, model = x_ref.shape[1:]
    length = len_ref[pl.program_id(0)]
    x_hat, _ = normalize(x_ref[0].astype(F32))
    h_one = (x_hat * vec_ref[4:5, :] + vec_ref[5:6, :]).astype(BF16)
    cos_tab, sin_tab = cos_ref[...], sin_ref[...]
    for i, out in enumerate((q_ref, k_ref)):
        proj = mm(h_one, w_ref[:, i * 64:(i + 1) * 64, :].reshape(model, model)) + vec_ref[i:i + 1, :]
        if i == 0:
            proj = proj * (HEAD_DIM ** -0.5)
        for g in range(model // GROUP):
            lo = g * GROUP
            first, second = rot_halves(proj[:, lo:lo + 128], proj[:, lo + 128:lo + 256], cos_tab, sin_tab)
            out[0, :, lo:lo + 128] = first.astype(BF16)
            out[0, :, lo + 128:lo + 256] = second.astype(BF16)
    proj = mm(h_one, w_ref[:, 128:192, :].reshape(model, model)) + vec_ref[2:3, :]
    v_ref[0] = proj.astype(BF16)
    qk_masks, vo_masks = head_masks()

    def attend(width):
        valid = lax.broadcasted_iota(jnp.int32, (1, width), 1) < length
        for g in range(model // GROUP):
            lo = g * GROUP
            k_cat = stack_masked(k_ref[0, 0:width, lo:lo + GROUP], qk_masks)
            scores = mm(q_ref[0, :, lo:lo + GROUP], k_cat, NT)
            probs = []
            for h in range(HEADS_GROUP):
                s_h = jnp.where(valid, scores[:, h * width:(h + 1) * width], NEG_BIG)
                e_h = jnp.exp(s_h - jnp.max(s_h, axis=-1, keepdims=True))
                p_h = (e_h * (1.0 / jnp.sum(e_h, axis=-1, keepdims=True))).astype(BF16)
                base = (g * HEADS_GROUP + h) * seq_len
                p_ref[0, :, base:base + width] = p_h
                probs.append(p_h)
            v_cat = stack_masked(v_ref[0, 0:width, lo:lo + GROUP], vo_masks)
            ctx_ref[0, :, lo:lo + GROUP] = mm(jnp.concatenate(probs, axis=1), v_cat).astype(BF16)

    for_key_width(length, seq_len, attend)
    attn_out = mm(ctx_ref[0], w_ref[:, 192:256, :].reshape(model, model))
    mid_ref[0] = (x_ref[0].astype(F32) + attn_out + vec_ref[3:4, :]).astype(BF16)


def mlp_fwd_kernel(mid_ref, w_ref, vec_ref, y_ref, act_ref, slope_ref):
    model = mid_ref.shape[1]
    mid = mid_ref[...].astype(F32)
    x_hat, _ = normalize(mid)
    h_two = (x_hat * vec_ref[6:7, :] + vec_ref[7:8, :]).astype(BF16)
    for c in range(4):
        cols = slice(c * model, (c + 1) * model)
        pre = mm(h_two, w_ref[:, c * 64:(c + 1) * 64, :].reshape(model, model)) + vec_ref[9 + c:10 + c, :]
        cdf = 0.5 * lax.erf(pre * (1.0 / math.sqrt(2.0))) + 0.5
        density = jnp.exp(pre * pre * -0.5) * (1.0 / math.sqrt(2.0 * math.pi))
        act_ref[:, cols] = (pre * cdf).astype(BF16)
        slope_ref[:, cols] = cdf + pre * density
    out = mm(act_ref[...], w_ref[:, 256:512, :].reshape(4 * model, model))
    y_ref[...] = (mid + out + vec_ref[8:9, :]).astype(BF16)


def mlp_bwd_kernel(dout_ref, mid_ref, act_ref, slope_ref, w_ref, vec_ref, dmid_ref, gw_ref, gs_ref, dpre_ref):
    model = mid_ref.shape[1]

    @pl.when(pl.program_id(0) == 0)
    def _():
        gw_ref[...] = jnp.zeros_like(gw_ref)
        gs_ref[...] = jnp.zeros_like(gs_ref)

    x_hat, rstd = normalize(mid_ref[...].astype(F32))
    h_two = (x_hat * vec_ref[6:7, :] + vec_ref[7:8, :]).astype(BF16)
    d_out = dout_ref[...]
    d_h = None
    for c in range(4):
        cols = slice(c * model, (c + 1) * model)
        d_act = mm(d_out, w_ref[2 * c:2 * c + 2, 256:512, :].reshape(model, model), NT)
        d_pre = d_act * slope_ref[:, cols]
        gs_ref[c:c + 1, :] += jnp.sum(d_pre, axis=0, keepdims=True)
        dpre_ref[:, cols] = d_pre.astype(BF16)
    for c in range(4):
        cols = slice(c * model, (c + 1) * model)
        gw_ref[2 * c:2 * c + 2, 256:512, :] += mm(act_ref[:, cols], d_out, TN).reshape(2, 256, model)
        gw_ref[:, c * 64:(c + 1) * 64, :] += mm(h_two, dpre_ref[:, cols], TN).reshape(8, 64, model)
        part = mm(dpre_ref[:, cols], w_ref[:, c * 64:(c + 1) * 64, :].reshape(model, model), NT)
        d_h = part if d_h is None else d_h + part
    d_out_f32 = d_out.astype(F32)
    gs_ref[4:5, :] += jnp.sum(d_out_f32, axis=0, keepdims=True)
    gs_ref[5:6, :] += jnp.sum(d_h * x_hat, axis=0, keepdims=True)
    gs_ref[6:7, :] += jnp.sum(d_h, axis=0, keepdims=True)
    dmid_ref[...] = (d_out_f32 + norm_bwd(d_h, x_hat, rstd, vec_ref[6:7, :])).astype(BF16)


def attn_bwd_kernel(len_ref, dmid_ref, x_ref, q_ref, k_ref, v_ref, p_ref, ctx_ref, w_ref, vec_ref, cos_ref, sin_ref,
                    dx_ref, gw_ref, gs_ref, dctx_ref, dq_ref, dk_ref, dv_ref):
    seq_len, model = x_ref.shape[1:]
    length = len_ref[pl.program_id(0)]

    @pl.when(pl.program_id(0) == 0)
    def _():
        gw_ref[...] = jnp.zeros_like(gw_ref)
        gs_ref[...] = jnp.zeros_like(gs_ref)

    d_mid = dmid_ref[0]
    d_mid_f32 = d_mid.astype(F32)
    gs_ref[3:4, :] += jnp.sum(d_mid_f32, axis=0, keepdims=True)
    gw_ref[:, 192:256, :] += mm(ctx_ref[0], d_mid, TN).reshape(8, 64, model)
    dctx_ref[...] = mm(d_mid, w_ref[:, 192:256, :].reshape(model, model), NT).astype(BF16)
    qk_masks, vo_masks = head_masks()

    def attend(width):
        for g in range(model // GROUP):
            lo = g * GROUP
            d_ctx = dctx_ref[:, lo:lo + GROUP]
            d_probs = mm(d_ctx, stack_masked(v_ref[0, 0:width, lo:lo + GROUP], vo_masks), NT)
            ds_list, dst_list, pt_list = [], [], []
            for h in range(HEADS_GROUP):
                base = (g * HEADS_GROUP + h) * seq_len
                p_bf = p_ref[0, :, base:base + width]
                p_h = p_bf.astype(F32)
                dp_h = d_probs[:, h * width:(h + 1) * width]
                ds_h = (p_h * (dp_h - jnp.sum(dp_h * p_h, axis=-1, keepdims=True))).astype(BF16)
                ds_list.append(ds_h)
                dst_list.append(ds_h.T)
                pt_list.append(p_bf.T)
            k_cat = stack_masked(k_ref[0, 0:width, lo:lo + GROUP], qk_masks)
            dq_ref[:, lo:lo + GROUP] = mm(jnp.concatenate(ds_list, axis=1), k_cat)
            q_cat = stack_masked(q_ref[0, :, lo:lo + GROUP], qk_masks)
            dk_ref[0:width, lo:lo + GROUP] = mm(jnp.concatenate(dst_list, axis=1), q_cat)
            do_cat = stack_masked(d_ctx, vo_masks)
            dv_ref[0:width, lo:lo + GROUP] = mm(jnp.concatenate(pt_list, axis=1), do_cat)
        if width < seq_len:
            dk_ref[width:, :] = jnp.zeros((seq_len - width, model), F32)
            dv_ref[width:, :] = jnp.zeros((seq_len - width, model), F32)

    for_key_width(length, seq_len, attend)
    cos_tab, sin_tab = cos_ref[...], sin_ref[...]
    x_hat, rstd = normalize(x_ref[0].astype(F32))
    h_one = (x_hat * vec_ref[4:5, :] + vec_ref[5:6, :]).astype(BF16)
    d_h = None
    for i, src in enumerate((dq_ref, dk_ref, dv_ref)):
        if i < 2:
            pieces = []
            for g in range(model // GROUP):
                lo = g * GROUP
                pieces.extend(unrot_halves(src[:, lo:lo + 128], src[:, lo + 128:lo + 256], cos_tab, sin_tab))
            d_proj = jnp.concatenate(pieces, axis=1)
            if i == 0:
                d_proj = d_proj * (HEAD_DIM ** -0.5)
        else:
            d_proj = src[...]
        d_proj = d_proj.astype(BF16)
        gs_ref[i:i + 1, :] += jnp.sum(d_proj.astype(F32), axis=0, keepdims=True)
        gw_ref[:, i * 64:(i + 1) * 64, :] += mm(h_one, d_proj, TN).reshape(8, 64, model)
        part = mm(d_proj, w_ref[:, i * 64:(i + 1) * 64, :].reshape(model, model), NT)
        d_h = part if d_h is None else d_h + part
    gs_ref[4:5, :] += jnp.sum(d_h * x_hat, axis=0, keepdims=True)
    gs_ref[5:6, :] += jnp.sum(d_h, axis=0, keepdims=True)
    dx_ref[0] = (d_mid_f32 + norm_bwd(d_h, x_hat, rstd, vec_ref[4:5, :])).astype(BF16)


def seq_spec(*tail):
    return pl.BlockSpec((1,) + tail, lambda b, *_: (b,) + (0,) * len(tail))


def row_spec(rows, cols):
    return pl.BlockSpec((rows, cols), lambda b, *_: (b, 0))


def whole(shape):
    return pl.BlockSpec(shape, lambda *_: (0,) * len(shape))


def params():
    return pltpu.CompilerParams(dimension_semantics=('arbitrary',), vmem_limit_bytes=VMEM_BYTES)


def cost(flops, nbytes):
    return pl.CostEstimate(flops=int(flops), bytes_accessed=int(nbytes), transcendentals=0)


def sds(shape, dtype):
    return jax.ShapeDtypeStruct(shape, dtype)


def attn_forward(lengths, x, w, vec, tables):
    n, seq_len, model = x.shape
    heads = model // HEAD_DIM
    act = sds(x.shape, BF16)
    spec = seq_spec(seq_len, model)
    return pl.pallas_call(
        attn_fwd_kernel,
        grid_spec=pltpu.PrefetchScalarGridSpec(
            num_scalar_prefetch=1, grid=(n,),
            in_specs=[spec, whole((8, 256, model)), whole(vec.shape), whole(tables[0].shape), whole(tables[1].shape)],
            out_specs=[spec, spec, spec, seq_spec(seq_len, heads * seq_len), spec, spec]),
        out_shape=[act, act, act, sds((n, seq_len, heads * seq_len), BF16), act, act],
        compiler_params=params(), cost_estimate=cost(16e9, 40e6), name='attn_fwd',
    )(lengths, x, w, vec, *tables)


def mlp_forward(mid, w, vec, rows):
    tokens, model = mid.shape
    return pl.pallas_call(
        mlp_fwd_kernel, grid=(tokens // rows,),
        in_specs=[row_spec(rows, model), whole(w.shape), whole(vec.shape)],
        out_specs=[row_spec(rows, model), row_spec(rows, 4 * model), row_spec(rows, 4 * model)],
        out_shape=[sds(mid.shape, BF16), sds((tokens, 4 * model), BF16), sds((tokens, 4 * model), F32)],
        compiler_params=params(), cost_estimate=cost(13e9, 50e6), name='mlp_fwd',
    )(mid, w, vec)


def mlp_backward(d_out, mid, act, slope, w, vec, rows):
    tokens, model = mid.shape
    wide = row_spec(rows, 4 * model)
    return pl.pallas_call(
        mlp_bwd_kernel, grid=(tokens // rows,),
        in_specs=[row_spec(rows, model), row_spec(rows, model), wide, wide, whole(w.shape), whole(vec.shape)],
        out_specs=[row_spec(rows, model), whole(w.shape), whole((8, model))],
        out_shape=[sds(mid.shape, BF16), sds(w.shape, F32), sds((8, model), F32)],
        scratch_shapes=[pltpu.VMEM((rows, 4 * model), BF16)],
        compiler_params=params(), cost_estimate=cost(26e9, 60e6), name='mlp_bwd',
    )(d_out, mid, act, slope, w, vec)


def attn_backward(lengths, d_mid, x, saved, w, vec, tables):
    n, seq_len, model = x.shape
    heads = model // HEAD_DIM
    spec = seq_spec(seq_len, model)
    return pl.pallas_call(
        attn_bwd_kernel,
        grid_spec=pltpu.PrefetchScalarGridSpec(
            num_scalar_prefetch=1, grid=(n,),
            in_specs=[spec, spec, spec, spec, spec, seq_spec(seq_len, heads * seq_len), spec, whole((8, 256, model)),
                      whole(vec.shape), whole(tables[0].shape), whole(tables[1].shape)],
            out_specs=[spec, whole((8, 256, model)), whole((8, model))],
            scratch_shapes=[pltpu.VMEM((seq_len, model), BF16)] + [pltpu.VMEM((seq_len, model), F32)] * 3),
        out_shape=[sds(x.shape, BF16), sds((8, 256, model), F32), sds((8, model), F32)],
        compiler_params=params(), cost_estimate=cost(30e9, 50e6), name='attn_bwd',
    )(lengths, d_mid, x, *saved, w, vec, *tables)


def permute_cols(arr):
    lead = arr.shape[:-1]
    return arr.reshape(lead + (-1, HEADS_GROUP, 2, 32)).swapaxes(-3, -2).reshape(arr.shape)


def unpermute_cols(arr):
    lead = arr.shape[:-1]
    return arr.reshape(lead + (-1, 2, HEADS_GROUP, 32)).swapaxes(-3, -2).reshape(arr.shape)


MESH_ID = pl.DeviceIdType.MESH


def place():
    me = lax.axis_index('fsdp')
    core, x_bit, y_bit = lax.rem(me, 2), lax.rem(me // 2, 2), me // 4

    def rel(ry, rx, rc):
        return lax.rem(y_bit + ry, 2) * 4 + lax.rem(x_bit + rx, 2) * 2 + lax.rem(core + rc, 2)

    return rel


def greet(rel):
    barrier = pltpu.get_barrier_semaphore()
    for peer in (rel(0, 0, 1), rel(0, 1, 0), rel(1, 0, 0)):
        pl.semaphore_signal(barrier, inc=1, device_id=(peer,), device_id_type=MESH_ID)
    pl.semaphore_wait(barrier, 3)


def remote(src, dst, sems, i, peer):
    return pltpu.make_async_remote_copy(src_ref=src, dst_ref=dst, send_sem=sems[0].at[i], recv_sem=sems[1].at[i],
                                        device_id=(peer,), device_id_type=MESH_ID)


def gather_kernel(in_ref, out_ref, vec_ref, send_sem, recv_sem):
    rel = place()
    core, px, py = rel(0, 0, 1), rel(0, 1, 0), rel(1, 0, 0)
    me, diag = rel(0, 0, 0), rel(1, 1, 0)
    rows = in_ref.shape[0]
    half = (pl.ds(0, rows // 2), pl.ds(rows // 2, rows // 2))
    sems = (send_sem, recv_sem)
    greet(rel)

    def own(h, i, peer):
        return remote(in_ref.at[half[h]], out_ref.at[me, half[h]], sems, i, peer)

    def pass_on(slot, h, i, peer):
        return remote(out_ref.at[slot, half[h]], out_ref.at[slot, half[h]], sems, i, peer)

    to_x = {1: own(1, 0, px), 0: own(0, 1, px)}
    to_y = {0: own(0, 2, py), 1: own(1, 3, py)}
    to_core = {0: own(0, 4, core), 1: own(1, 5, core)}
    for copy in (to_x[1], to_y[0], to_x[0], to_y[1], to_core[0], to_core[1]):
        copy.start()
    out_ref[pl.ds(me, 1)] = in_ref[...][None]
    on_x = pass_on(py, 0, 6, px)
    on_y = pass_on(px, 1, 7, py)
    core_fwd = {('x', 1): pass_on(px, 1, 8, core), ('y', 0): pass_on(py, 0, 9, core),
                ('x', 0): pass_on(px, 0, 10, core), ('y', 1): pass_on(py, 1, 11, core),
                ('d', 0): pass_on(diag, 0, 12, core), ('d', 1): pass_on(diag, 1, 13, core)}
    to_y[0].wait_recv()
    on_x.start()
    to_x[1].wait_recv()
    on_y.start()
    core_fwd[('y', 0)].start()
    core_fwd[('x', 1)].start()
    to_x[0].wait_recv()
    core_fwd[('x', 0)].start()
    to_y[1].wait_recv()
    core_fwd[('y', 1)].start()
    on_x.wait_recv()
    core_fwd[('d', 0)].start()
    on_y.wait_recv()
    core_fwd[('d', 1)].start()
    for copy in (to_core[0], to_core[1]) + tuple(core_fwd.values()):
        copy.wait_recv()
    for copy in tuple(to_x.values()) + tuple(to_y.values()) + (on_x, on_y) + tuple(to_core.values()) + tuple(core_fwd.values()):
        copy.wait_send()
    total = out_ref[0, 256:288, :].astype(F32)
    for d in range(1, 8):
        total = total + out_ref[d, 256:288, :].astype(F32)
    vec_ref[...] = total.reshape(vec_ref.shape)


def gather_head(packed):
    rows, model = packed.shape
    vmem = pl.BlockSpec(memory_space=pltpu.VMEM)
    return pl.pallas_call(
        gather_kernel, in_specs=[vmem], out_specs=[vmem, vmem],
        out_shape=[sds((8, rows, model), BF16), sds((2, 16, model), F32)],
        scratch_shapes=[pltpu.SemaphoreType.DMA((14,)), pltpu.SemaphoreType.DMA((14,))],
        compiler_params=pltpu.CompilerParams(collective_id=0, has_side_effects=True, vmem_limit_bytes=VMEM_BYTES),
        cost_estimate=cost(1e9, 4e6), name='gather_head',
    )(packed)


PIECE = 64


def scatter_kernel(ga_ref, gb_ref, gs_ref, oa_ref, ob_ref, os_ref, r1, r2, r3, s2, s3, keep,
                   t1, t2, t3, u2, u3, keep_s, send1, recv1, send2, recv2, send3, recv3):
    rel = place()
    core, px, py = rel(0, 0, 1), rel(0, 1, 0), rel(1, 0, 0)
    greet(rel)
    pieces = []
    for src, out in ((ga_ref, oa_ref), (gb_ref, ob_ref)):
        for j in (0, 2, 1, 3):
            n = len(pieces)
            pieces.append((src, out, j * PIECE, PIECE, j < 2, r1.at[n], r2.at[n], r3.at[n], s2.at[n], s3.at[n], keep.at[n]))
    pieces.append((gs_ref, os_ref, 0, gs_ref.shape[1], True, t1, t2, t3, u2, u3, keep_s))

    first, second, third = [], [], []
    for n, (src, out, row, rows, x_first, b1, b2, b3, c2, c3, kp) in enumerate(pieces):
        copies = [remote(src.at[rel(r // 2, r % 2, 1), pl.ds(row, rows)], b1.at[r], (send1, recv1), 4 * n + r, core)
                  for r in range(4)]
        for copy in copies:
            copy.start()
        first.append(copies)
        second.append(remote(c2, b2, (send2, recv2), n, px if x_first else py))
        third.append(remote(c3, b3, (send3, recv3), n, py if x_first else px))
    for n, (src, out, row, rows, x_first, b1, b2, b3, c2, c3, kp) in enumerate(pieces):
        for copy in first[n]:
            copy.wait_recv()
        sent, kept = ((1, 3), (0, 2)) if x_first else ((2, 3), (0, 1))

        def total(r):
            return src[pl.ds(rel(r // 2, r % 2, 0), 1), row:row + rows, :][0] + b1[r]

        c2[0] = total(sent[0])
        c2[1] = total(sent[1])
        kp[0] = total(kept[0])
        kp[1] = total(kept[1])
        second[n].start()
    for n, (src, out, row, rows, x_first, b1, b2, b3, c2, c3, kp) in enumerate(pieces):
        second[n].wait_recv()
        c3[...] = kp[1] + b2[1]
        kp[0] = kp[0] + b2[0]
        third[n].start()
    for n, (src, out, row, rows, x_first, b1, b2, b3, c2, c3, kp) in enumerate(pieces):
        third[n].wait_recv()
        out[row:row + rows, :] = kp[0] + b3[...]
    for n in range(len(pieces)):
        for copy in first[n] + [second[n], third[n]]:
            copy.wait_send()


def scatter_tail(g_a, g_b, g_s):
    _, rows, model = g_a.shape
    small = g_s.shape[1]
    vmem = pl.BlockSpec(memory_space=pltpu.VMEM)
    n = 2 * rows // PIECE
    dma = pltpu.SemaphoreType.DMA
    return pl.pallas_call(
        scatter_kernel, in_specs=[vmem] * 3, out_specs=[vmem] * 3,
        out_shape=[sds((rows, model), F32), sds((rows, model), F32), sds((small, model), F32)],
        scratch_shapes=[pltpu.VMEM((n, 4, PIECE, model), F32), pltpu.VMEM((n, 2, PIECE, model), F32),
                        pltpu.VMEM((n, PIECE, model), F32), pltpu.VMEM((n, 2, PIECE, model), F32),
                        pltpu.VMEM((n, PIECE, model), F32), pltpu.VMEM((n, 2, PIECE, model), F32),
                        pltpu.VMEM((4, small, model), F32), pltpu.VMEM((2, small, model), F32),
                        pltpu.VMEM((small, model), F32), pltpu.VMEM((2, small, model), F32),
                        pltpu.VMEM((small, model), F32), pltpu.VMEM((2, small, model), F32),
                        dma((4 * n + 4,)), dma((4 * n + 4,)), dma((n + 1,)), dma((n + 1,)), dma((n + 1,)), dma((n + 1,))],
        compiler_params=pltpu.CompilerParams(collective_id=1, has_side_effects=True, vmem_limit_bytes=VMEM_BYTES),
        cost_estimate=cost(1e9, 8e6), name='scatter_tail',
    )(g_a, g_b, g_s)


def solution(mesh):
    axis = mesh.axis_names[0]
    batch_spec = P(axis)
    weight_specs = (P(None, None, axis, None), P(None, None, axis), P(None, None, axis),
                    P(None, axis, None), P(None, axis), P(None, axis, None), P(None, axis))

    def device_step(x, lengths, d_y, w_attn, b_attn, ln_par, w_up, b_up, w_down, b_down):
        n_layers, _, part, model = w_attn.shape
        n_seq, seq_len = x.shape[:2]
        tables = rotary_tables(seq_len)
        rows = 384

        def gather(a):
            return lax.all_gather(a, axis, axis=0, tiled=False)

        mine = (jnp.arange(8) == lax.axis_index(axis)).astype(BF16)
        nine = jnp.concatenate([b_attn, ln_par, b_down[:, None, :]], axis=1)
        nine = (nine[:, :, None, :] * mine[None, None, :, None]).reshape(n_layers, 9, model)
        up = (b_up[:, None, :] * mine[None, :, None]).reshape(n_layers, 4, model)
        small = jnp.concatenate([permute_cols(nine[:, :2]), nine[:, 2:], up, jnp.zeros((n_layers, 3, model), BF16)], axis=1)
        attn_shards = [jnp.concatenate([permute_cols(w_attn[l, :2]), w_attn[l, 2:]], axis=0).reshape(4 * part, model)
                       for l in range(n_layers)]
        head, vec_all = gather_head(jnp.concatenate([attn_shards[0], small.reshape(n_layers * 16, model)], axis=0))
        vecs = [vec_all[l] for l in range(n_layers)]
        mlp_shards = [jnp.concatenate([w_up[l].reshape(part, 4, model).swapaxes(0, 1).reshape(4 * part, model), w_down[l]], axis=0)
                      for l in range(n_layers)]
        mlp_w0 = gather(mlp_shards[0])
        attn_w1 = gather(attn_shards[1])
        mlp_w1 = gather(mlp_shards[1])
        attn_w = [head, attn_w1]
        mlp_w = [mlp_w0, mlp_w1]

        hidden = x
        saved = []
        for l in range(n_layers):
            q, k, v, probs, ctx, mid = attn_forward(lengths, hidden, attn_w[l], vecs[l], tables)
            mid2 = mid.reshape(n_seq * seq_len, model)
            y, act, slope = mlp_forward(mid2, mlp_w[l], vecs[l], rows)
            saved.append((hidden, (q, k, v, probs, ctx), mid2, act, slope))
            hidden = y.reshape(x.shape)

        grad = d_y.reshape(n_seq * seq_len, model)
        g_attn, g_mlp, g_small = [None] * n_layers, [None] * n_layers, [None] * n_layers
        for l in reversed(range(n_layers)):
            x_in, attn_saved, mid2, act, slope = saved[l]
            d_mid, gw_mlp, gs_mlp = mlp_backward(grad, mid2, act, slope, mlp_w[l], vecs[l], rows)
            g_mlp[l] = lax.psum_scatter(gw_mlp, axis, scatter_dimension=0, tiled=False)
            d_x, gw_attn, gs_attn = attn_backward(lengths, d_mid.reshape(x.shape), x_in, attn_saved, attn_w[l], vecs[l], tables)
            g_attn[l] = gw_attn
            grad = d_x.reshape(n_seq * seq_len, model)
            gqk = unpermute_cols(gs_attn[:2])
            nine = jnp.concatenate([gqk, gs_attn[2:6], gs_mlp[5:7], gs_mlp[4:5]], axis=0)
            nine = nine.reshape(9, 8, part).swapaxes(0, 1)
            g_small[l] = jnp.concatenate([nine, gs_mlp[:4].reshape(8, 4, part)], axis=1)
        small_part = jnp.stack(g_small, axis=1).reshape(8, -1)
        small_part = jnp.pad(small_part, ((0, 0), (0, 8 * model - small_part.shape[1]))).reshape(8, 8, model)
        sum_1, sum_0, small_sum = scatter_tail(g_attn[1], g_attn[0], small_part)
        small_sum = small_sum.reshape(-1)[:n_layers * 13 * part].reshape(n_layers, 13, part)
        g_a = jnp.stack([sum_0, sum_1]).reshape(n_layers, 4, part, model)
        g_a = jnp.concatenate([unpermute_cols(g_a[:, :2]), g_a[:, 2:]], axis=1)
        g_m = jnp.stack(g_mlp)
        g_up = g_m[:, :4 * part].reshape(n_layers, 4, part, model).swapaxes(1, 2).reshape(n_layers, part, 4 * model)
        g_down = g_m[:, 4 * part:]
        return (grad.reshape(x.shape), g_a, small_sum[:, 0:4], small_sum[:, 4:8], g_up,
                small_sum[:, 9:13].reshape(n_layers, 4 * part), g_down, small_sum[:, 8])

    return jax.shard_map(device_step, mesh=mesh,
                         in_specs=(batch_spec, batch_spec, batch_spec) + weight_specs,
                         out_specs=(batch_spec,) + weight_specs,
                         check_vma=False)
```

```python
import math
import jax
import jax.numpy as jnp
from jax import lax
from jax.experimental import pallas as pl
from jax.experimental.pallas import tpu as pltpu
from jax.sharding import PartitionSpec as P

HEAD_DIM = 64
EPS = 1e-5
THETA = 10000.0
NEG_BIG = -1e30
BF16 = jnp.bfloat16
F32 = jnp.float32
VMEM_BYTES = 60 * 1024 * 1024
GROUP = 256
HEADS_GROUP = 4
KEY_BLOCK = 128
FWD_ROWS = 384
BWD_ROWS = 512

NN, NT, TN = (1, 0), (1, 1), (0, 0)


def mm(a, b, dims=NN):
    return lax.dot_general(a, b, (((dims[0],), (dims[1],)), ((), ())), preferred_element_type=F32)


def line(ref, i):
    return ref[i:i + 1, :]


def add_line(ref, i, block):
    ref[i:i + 1, :] += jnp.sum(block, axis=0, keepdims=True)


def row_mean(block):
    return jnp.mean(block, axis=-1, keepdims=True)


def row_sum(block):
    return jnp.sum(block, axis=-1, keepdims=True)


def square(w_ref, i):
    model = w_ref.shape[-1]
    return w_ref[:, i * HEAD_DIM:(i + 1) * HEAD_DIM, :].reshape(model, model)


def rotary_tables(seq_len):
    half_dim = HEAD_DIM // 2
    freq_pos = (jnp.arange(2 * HEAD_DIM) % half_dim).astype(F32)
    inv_freq = 1.0 / (THETA ** (freq_pos * (2.0 / HEAD_DIM)))
    angles = jnp.arange(seq_len, dtype=F32)[:, None] * inv_freq[None, :]
    return jnp.cos(angles), jnp.sin(angles)


def normalize(x_f32):
    centered = x_f32 - row_mean(x_f32)
    rstd = lax.rsqrt(row_mean(centered * centered) + EPS)
    return centered * rstd, rstd


def norm_bwd(d_h, x_hat, rstd, gain):
    d_hat = d_h * gain
    mean_d = row_mean(d_hat)
    mean_dx = row_mean(d_hat * x_hat)
    return rstd * (d_hat - mean_d - x_hat * mean_dx)


def halves(block, lo):
    mid = lo + GROUP // 2
    return block[:, lo:mid], block[:, mid:lo + GROUP]


def rot_halves(first, second, cos_tab, sin_tab):
    return first * cos_tab - second * sin_tab, second * cos_tab + first * sin_tab


def unrot_halves(first, second, cos_tab, sin_tab):
    return first * cos_tab + second * sin_tab, second * cos_tab - first * sin_tab


def head_masks():
    lane = lax.broadcasted_iota(jnp.int32, (1, GROUP), 1)
    qk = [((lane % 128) // 32 == h).astype(F32).astype(BF16) for h in range(HEADS_GROUP)]
    vo = [(lane // 64 == h).astype(F32).astype(BF16) for h in range(HEADS_GROUP)]
    return qk, vo


def stack_masked(block, masks):
    return jnp.concatenate([block * m for m in masks], axis=0)


def for_key_width(length, seq_len, body):
    blocks = (length + KEY_BLOCK - 1) // KEY_BLOCK
    for n in range(1, seq_len // KEY_BLOCK + 1):
        @pl.when(blocks == n)
        def _(n=n):
            body(n * KEY_BLOCK)


def attn_fwd_kernel(len_ref, x_ref, w_ref, vec_ref, cos_ref, sin_ref, q_ref, k_ref, v_ref, p_ref, ctx_ref, mid_ref):
    seq_len, model = x_ref.shape[1:]
    length = len_ref[pl.program_id(0)]
    x_hat, _ = normalize(x_ref[0].astype(F32))
    h_one = (x_hat * line(vec_ref, 4) + line(vec_ref, 5)).astype(BF16)
    cos_tab, sin_tab = cos_ref[:], sin_ref[:]
    for i, out in enumerate((q_ref, k_ref)):
        proj = mm(h_one, square(w_ref, i)) + line(vec_ref, i)
        if i == 0:
            proj = proj * (HEAD_DIM ** -0.5)
        for g in range(model // GROUP):
            lo = g * GROUP
            first, second = rot_halves(*halves(proj, lo), cos_tab, sin_tab)
            out[0, :, lo:lo + GROUP] = jnp.concatenate([first.astype(BF16), second.astype(BF16)], axis=1)
    proj = mm(h_one, square(w_ref, 2)) + line(vec_ref, 2)
    v_ref[0] = proj.astype(BF16)
    qk_masks, vo_masks = head_masks()

    def attend(width):
        valid = lax.broadcasted_iota(jnp.int32, (1, width), 1) < length
        for g in range(model // GROUP):
            lo = g * GROUP
            k_cat = stack_masked(k_ref[0, 0:width, lo:lo + GROUP], qk_masks)
            scores = mm(q_ref[0, :, lo:lo + GROUP], k_cat, NT)
            probs = []
            for h in range(HEADS_GROUP):
                s_h = jnp.where(valid, scores[:, h * width:(h + 1) * width], NEG_BIG)
                e_h = jnp.exp(s_h - jnp.max(s_h, axis=-1, keepdims=True))
                p_h = (e_h * (1.0 / row_sum(e_h))).astype(BF16)
                base = (g * HEADS_GROUP + h) * seq_len
                p_ref[0, :, base:base + width] = p_h
                probs.append(p_h)
            v_cat = stack_masked(v_ref[0, 0:width, lo:lo + GROUP], vo_masks)
            ctx_ref[0, :, lo:lo + GROUP] = mm(jnp.concatenate(probs, axis=1), v_cat).astype(BF16)

    for_key_width(length, seq_len, attend)
    attn_out = mm(ctx_ref[0], square(w_ref, 3))
    mid_ref[0] = (x_ref[0].astype(F32) + attn_out + line(vec_ref, 3)).astype(BF16)


def mlp_fwd_kernel(mid_ref, w_ref, vec_ref, y_ref, act_ref, slope_ref):
    model = mid_ref.shape[1]
    mid = mid_ref[:].astype(F32)
    x_hat, _ = normalize(mid)
    h_two = (x_hat * line(vec_ref, 6) + line(vec_ref, 7)).astype(BF16)
    for c in range(4):
        cols = slice(c * model, (c + 1) * model)
        pre = mm(h_two, square(w_ref, c)) + line(vec_ref, 9 + c)
        cdf = 0.5 * lax.erf(pre * (1.0 / math.sqrt(2.0))) + 0.5
        density = jnp.exp(pre * pre * -0.5) * (1.0 / math.sqrt(2.0 * math.pi))
        act_ref[:, cols] = (pre * cdf).astype(BF16)
        slope_ref[:, cols] = cdf + pre * density
    out = mm(act_ref[:], w_ref[:, 256:512, :].reshape(4 * model, model))
    y_ref[:] = (mid + out + line(vec_ref, 8)).astype(BF16)


def mlp_bwd_scatter_kernel(dout_ref, mid_ref, act_ref, slope_ref, w_ref, vec_ref, ga_ref, dmid_ref, gw_ref, gs_ref, out_ref,
                           dpre_ref, own_ref, *rest):
    job = Scatter(ga_ref, own_ref, out_ref, rest[:6], rest[6:])
    step, last = pl.program_id(0), pl.num_programs(0) - 1
    pl.when(step == 0)(job.stage_one)
    pl.when(step == 1)(job.stage_two)
    pl.when(step == last - 1)(job.stage_three)
    mlp_bwd_kernel(dout_ref, mid_ref, act_ref, slope_ref, w_ref, vec_ref, dmid_ref, gw_ref, gs_ref, dpre_ref)
    pl.when(step == last)(job.stage_four)


def mlp_bwd_kernel(dout_ref, mid_ref, act_ref, slope_ref, w_ref, vec_ref, dmid_ref, gw_ref, gs_ref, dpre_ref):
    model = mid_ref.shape[1]

    @pl.when(pl.program_id(0) == 0)
    def _():
        gw_ref[:] = jnp.zeros_like(gw_ref)
        gs_ref[:] = jnp.zeros_like(gs_ref)

    x_hat, rstd = normalize(mid_ref[:].astype(F32))
    h_two = (x_hat * line(vec_ref, 6) + line(vec_ref, 7)).astype(BF16)
    d_out = dout_ref[:]
    d_h = None
    for c in range(4):
        cols = slice(c * model, (c + 1) * model)
        d_act = mm(d_out, w_ref[2 * c:2 * c + 2, 256:512, :].reshape(model, model), NT)
        d_pre = d_act * slope_ref[:, cols]
        add_line(gs_ref, c, d_pre)
        dpre_ref[:, cols] = d_pre.astype(BF16)
    for c in range(4):
        cols = slice(c * model, (c + 1) * model)
        gw_ref[2 * c:2 * c + 2, 256:512, :] += mm(act_ref[:, cols], d_out, TN).reshape(2, 256, model)
        gw_ref[:, c * 64:(c + 1) * 64, :] += mm(h_two, dpre_ref[:, cols], TN).reshape(8, 64, model)
        part = mm(dpre_ref[:, cols], square(w_ref, c), NT)
        d_h = part if d_h is None else d_h + part
    d_out_f32 = d_out.astype(F32)
    add_line(gs_ref, 4, d_out_f32)
    add_line(gs_ref, 5, d_h * x_hat)
    add_line(gs_ref, 6, d_h)
    dmid_ref[:] = (d_out_f32 + norm_bwd(d_h, x_hat, rstd, line(vec_ref, 6))).astype(BF16)


def attn_bwd_kernel(len_ref, dmid_ref, x_ref, q_ref, k_ref, v_ref, p_ref, ctx_ref, w_ref, vec_ref, cos_ref, sin_ref,
                    dx_ref, gw_ref, gs_ref, dctx_ref, dq_ref, dk_ref, dv_ref):
    seq_len, model = x_ref.shape[1:]
    length = len_ref[pl.program_id(0)]

    @pl.when(pl.program_id(0) == 0)
    def _():
        gw_ref[:] = jnp.zeros_like(gw_ref)
        gs_ref[:] = jnp.zeros_like(gs_ref)

    d_mid = dmid_ref[0]
    d_mid_f32 = d_mid.astype(F32)
    add_line(gs_ref, 3, d_mid_f32)
    gw_ref[:, 192:256, :] += mm(ctx_ref[0], d_mid, TN).reshape(8, 64, model)
    dctx_ref[:] = mm(d_mid, square(w_ref, 3), NT).astype(BF16)
    qk_masks, vo_masks = head_masks()

    def attend(width):
        for g in range(model // GROUP):
            lo = g * GROUP
            d_ctx = dctx_ref[:, lo:lo + GROUP]
            d_probs = mm(d_ctx, stack_masked(v_ref[0, 0:width, lo:lo + GROUP], vo_masks), NT)
            ds_list, dst_list, pt_list = [], [], []
            for h in range(HEADS_GROUP):
                base = (g * HEADS_GROUP + h) * seq_len
                p_bf = p_ref[0, :, base:base + width]
                p_h = p_bf.astype(F32)
                dp_h = d_probs[:, h * width:(h + 1) * width]
                ds_h = (p_h * (dp_h - row_sum(dp_h * p_h))).astype(BF16)
                ds_list.append(ds_h)
                dst_list.append(ds_h.T)
                pt_list.append(p_bf.T)
            k_cat = stack_masked(k_ref[0, 0:width, lo:lo + GROUP], qk_masks)
            dq_ref[:, lo:lo + GROUP] = mm(jnp.concatenate(ds_list, axis=1), k_cat)
            q_cat = stack_masked(q_ref[0, :, lo:lo + GROUP], qk_masks)
            dk_ref[0:width, lo:lo + GROUP] = mm(jnp.concatenate(dst_list, axis=1), q_cat)
            do_cat = stack_masked(d_ctx, vo_masks)
            dv_ref[0:width, lo:lo + GROUP] = mm(jnp.concatenate(pt_list, axis=1), do_cat)
        if width < seq_len:
            dk_ref[width:, :] = jnp.zeros((seq_len - width, model), F32)
            dv_ref[width:, :] = jnp.zeros((seq_len - width, model), F32)

    for_key_width(length, seq_len, attend)
    cos_tab, sin_tab = cos_ref[:], sin_ref[:]
    x_hat, rstd = normalize(x_ref[0].astype(F32))
    h_one = (x_hat * line(vec_ref, 4) + line(vec_ref, 5)).astype(BF16)
    d_h = None
    for i, src in enumerate((dq_ref, dk_ref, dv_ref)):
        if i < 2:
            pieces = []
            for g in range(model // GROUP):
                lo = g * GROUP
                pieces.extend(unrot_halves(*halves(src, lo), cos_tab, sin_tab))
            d_proj = jnp.concatenate(pieces, axis=1)
            if i == 0:
                d_proj = d_proj * (HEAD_DIM ** -0.5)
        else:
            d_proj = src[:]
        d_proj = d_proj.astype(BF16)
        add_line(gs_ref, i, d_proj.astype(F32))
        gw_ref[:, i * 64:(i + 1) * 64, :] += mm(h_one, d_proj, TN).reshape(8, 64, model)
        part = mm(d_proj, square(w_ref, i), NT)
        d_h = part if d_h is None else d_h + part
    add_line(gs_ref, 4, d_h * x_hat)
    add_line(gs_ref, 5, d_h)
    dx_ref[0] = (d_mid_f32 + norm_bwd(d_h, x_hat, rstd, line(vec_ref, 4))).astype(BF16)


def seq_spec(*tail):
    return pl.BlockSpec((1,) + tail, lambda b, *_: (b,) + (0,) * len(tail))


def row_spec(rows, cols):
    return pl.BlockSpec((rows, cols), lambda b, *_: (b, 0))


def whole(shape):
    return pl.BlockSpec(shape, lambda *_: (0,) * len(shape))


def params():
    return pltpu.CompilerParams(dimension_semantics=('arbitrary',), vmem_limit_bytes=VMEM_BYTES)


def cost(flops, nbytes):
    return pl.CostEstimate(flops=int(flops), bytes_accessed=int(nbytes), transcendentals=0)


def sds(shape, dtype):
    return jax.ShapeDtypeStruct(shape, dtype)


def attn_forward(lengths, x, w, vec, tables):
    n, seq_len, model = x.shape
    heads = model // HEAD_DIM
    act = sds(x.shape, BF16)
    spec = seq_spec(seq_len, model)
    return pl.pallas_call(
        attn_fwd_kernel,
        grid_spec=pltpu.PrefetchScalarGridSpec(
            num_scalar_prefetch=1, grid=(n,),
            in_specs=[spec, whole((8, 256, model)), whole(vec.shape), whole(tables[0].shape), whole(tables[1].shape)],
            out_specs=[spec, spec, spec, seq_spec(seq_len, heads * seq_len), spec, spec]),
        out_shape=[act, act, act, sds((n, seq_len, heads * seq_len), BF16), act, act],
        compiler_params=params(), cost_estimate=cost(16e9, 40e6), name='attn_fwd',
    )(lengths, x, w, vec, *tables)


def mlp_forward(mid, w, vec, rows):
    tokens, model = mid.shape
    return pl.pallas_call(
        mlp_fwd_kernel, grid=(tokens // rows,),
        in_specs=[row_spec(rows, model), whole(w.shape), whole(vec.shape)],
        out_specs=[row_spec(rows, model), row_spec(rows, 4 * model), row_spec(rows, 4 * model)],
        out_shape=[sds(mid.shape, BF16), sds((tokens, 4 * model), BF16), sds((tokens, 4 * model), F32)],
        compiler_params=params(), cost_estimate=cost(13e9, 50e6), name='mlp_fwd',
    )(mid, w, vec)


def mlp_backward(d_out, mid, act, slope, w, vec, rows, g_a=None):
    tokens, model = mid.shape
    wide = row_spec(rows, 4 * model)
    in_specs = [row_spec(rows, model), row_spec(rows, model), wide, wide, whole(w.shape), whole(vec.shape)]
    out_specs = [row_spec(rows, model), whole(w.shape), whole((8, model))]
    out_shape = [sds(mid.shape, BF16), sds(w.shape, F32), sds((8, model), F32)]
    scratch = [pltpu.VMEM((rows, 4 * model), BF16)]
    ins, kernel, extra = (d_out, mid, act, slope, w, vec), mlp_bwd_kernel, {}
    if g_a is not None:
        ins, kernel, extra = ins + (g_a,), mlp_bwd_scatter_kernel, {'collective_id': 2, 'has_side_effects': True}
        in_specs.append(pl.BlockSpec(memory_space=pl.ANY))
        out_specs.append(whole(g_a.shape[1:]))
        out_shape.append(sds(g_a.shape[1:], F32))
        n = g_a.shape[1] // PIECE
        scratch += [pltpu.VMEM((4,) + g_a.shape[1:], F32)] + scatter_bufs(n, PIECE, model) + scatter_sems(n)
    return pl.pallas_call(
        kernel, grid=(tokens // rows,), in_specs=in_specs, out_specs=out_specs, out_shape=out_shape, scratch_shapes=scratch,
        compiler_params=pltpu.CompilerParams(dimension_semantics=('arbitrary',), vmem_limit_bytes=VMEM_BYTES, **extra),
        cost_estimate=cost(26e9, 60e6), name='mlp_bwd',
    )(*ins)


def attn_backward(lengths, d_mid, x, saved, w, vec, tables):
    n, seq_len, model = x.shape
    heads = model // HEAD_DIM
    spec = seq_spec(seq_len, model)
    return pl.pallas_call(
        attn_bwd_kernel,
        grid_spec=pltpu.PrefetchScalarGridSpec(
            num_scalar_prefetch=1, grid=(n,),
            in_specs=[spec, spec, spec, spec, spec, seq_spec(seq_len, heads * seq_len), spec, whole((8, 256, model)),
                      whole(vec.shape), whole(tables[0].shape), whole(tables[1].shape)],
            out_specs=[spec, whole((8, 256, model)), whole((8, model))],
            scratch_shapes=[pltpu.VMEM((seq_len, model), BF16)] + [pltpu.VMEM((seq_len, model), F32)] * 3),
        out_shape=[sds(x.shape, BF16), sds((8, 256, model), F32), sds((8, model), F32)],
        compiler_params=params(), cost_estimate=cost(30e9, 50e6), name='attn_bwd',
    )(lengths, d_mid, x, *saved, w, vec, *tables)


MESH_ID = pl.DeviceIdType.MESH
PIECE = 64
SMALL = 32


def place():
    me = lax.axis_index('fsdp')
    core, x_bit, y_bit = lax.rem(me, 2), lax.rem(me // 2, 2), me // 4

    def rel(ry, rx, rc):
        return lax.rem(y_bit + ry, 2) * 4 + lax.rem(x_bit + rx, 2) * 2 + lax.rem(core + rc, 2)

    return rel


def peers(rel):
    return rel(0, 0, 1), rel(0, 1, 0), rel(1, 0, 0)


def greet(targets):
    barrier = pltpu.get_barrier_semaphore()
    for peer in targets:
        pl.semaphore_signal(barrier, device_id=(peer,), device_id_type=MESH_ID)
    pl.semaphore_wait(barrier, len(targets))


def remote(src, dst, sems, i, peer):
    return pltpu.make_async_remote_copy(src_ref=src, dst_ref=dst, send_sem=sems[0].at[i], recv_sem=sems[1].at[i],
                                        device_id=(peer,), device_id_type=MESH_ID)


def pack_small(dst, me, perm, b_attn, ln_par, b_up, b_down):
    part, model = b_attn.shape[-1], dst.shape[-1]
    spot = (lax.broadcasted_iota(jnp.int32, (part, model), 1) == lax.broadcasted_iota(jnp.int32, (part, model), 0) + me * part)
    spot = spot.astype(F32).astype(BF16)
    lane = lax.broadcasted_iota(jnp.int32, (4, model), 1)
    row = lax.broadcasted_iota(jnp.int32, (4, model), 0)
    here = (row == me // 2) & (lane // GROUP == lax.rem(me, 2))
    dst[:] = jnp.zeros_like(dst)
    for l in range(b_attn.shape[0]):
        base = l * SMALL // 2
        bias = mm(b_attn[l], spot)
        dst[base:base + 2, :] = permute_mm(bias[:2].astype(BF16), perm)
        dst[base + 2:base + 4, :] = bias[2:]
        dst[base + 4:base + 8, :] = mm(ln_par[l], spot)
        dst[base + 8:base + 9, :] = mm(b_down[l:l + 1, :], spot)
        up = b_up[l:l + 1, :].astype(F32)
        dst[base + 9:base + 13, :] = jnp.where(here, jnp.concatenate([up, up], axis=1), 0.0)


def permutation():
    old = lax.broadcasted_iota(jnp.int32, (GROUP, GROUP), 0)
    new = lax.broadcasted_iota(jnp.int32, (GROUP, GROUP), 1)
    half = HEAD_DIM // 2
    want = (new % 128) // half * HEAD_DIM + new // 128 * half + new % half
    return (old == want).astype(F32).astype(BF16)


def permute_mm(block, perm):
    return jnp.concatenate([mm(block[:, lo:lo + GROUP], perm) for lo in range(0, block.shape[1], GROUP)], axis=1)


def pack_attn(write, w_layer, perm):
    part = w_layer.shape[1]
    for i in range(4):
        rows = w_layer[i]
        write(slice(i * part, (i + 1) * part), permute_mm(rows, perm).astype(BF16) if i < 2 else rows)


def gather_kernel(w_attn, b_attn, ln_par, w_up, b_up, w_down, b_down, out_ref, vec0_ref, vec1_ref, attn_ref, mlp0_ref, mlp1_ref,
                  pack_ref, small_ref, send_sem, recv_sem):
    rel = place()
    core, px, py = peers(rel)
    me, diag = rel(0, 0, 0), rel(1, 1, 0)
    part, model = w_attn.shape[2:]
    perm = permutation()

    def put(rows, value):
        pack_ref[rows, :] = value

    def put_second(rows, value):
        attn_ref[rows, :] = value

    pack_small(small_ref, me, perm, b_attn, ln_par, b_up, b_down)
    pack_ref[4 * part:, :] = small_ref[:].astype(BF16)
    pack_attn(put, w_attn[0], perm)
    rows = pack_ref.shape[0]
    top, low = pl.ds(0, rows // 2), pl.ds(rows // 2, rows // 2)
    sems = (send_sem, recv_sem)
    greet((core, px, py))

    ids = iter(range(send_sem.shape[0]))

    def own(rows, peer):
        return remote(pack_ref.at[rows], out_ref.at[me, rows], sems, next(ids), peer)

    def pass_on(slot, rows, peer):
        return remote(out_ref.at[slot, rows], out_ref.at[slot, rows], sems, next(ids), peer)

    x_late, x_soon = own(top, px), own(low, px)
    y_soon, y_late = own(top, py), own(low, py)
    c_one, c_two = own(top, core), own(low, core)
    for copy in (x_soon, y_soon, x_late, y_late, c_one, c_two):
        copy.start()
    out_ref[pl.ds(me, 1)] = pack_ref[:][None]
    pack_attn(put_second, w_attn[1], perm)
    for l, mlp_ref in enumerate((mlp0_ref, mlp1_ref)):
        for c in range(4):
            mlp_ref[c * part:(c + 1) * part, :] = w_up[l, :, c * model:(c + 1) * model]
        mlp_ref[4 * part:, :] = w_down[l]
    on_x, on_y = pass_on(py, top, px), pass_on(px, low, py)
    steps = [(y_soon, on_x, pass_on(py, top, core)), (x_soon, on_y, pass_on(px, low, core)),
             (x_late, None, pass_on(px, top, core)), (y_late, None, pass_on(py, low, core)),
             (on_x, None, pass_on(diag, top, core)), (on_y, None, pass_on(diag, low, core))]
    for arrived, onward, across in steps:
        arrived.wait_recv()
        if onward:
            onward.start()
        across.start()
    from_core = [c_one, c_two] + [across for _, _, across in steps]
    for copy in from_core:
        copy.wait_recv()
    for copy in from_core + [arrived for arrived, _, _ in steps]:
        copy.wait_send()
    total = sum(out_ref[d, 4 * part:, :].astype(F32) for d in range(8))
    vec0_ref[:] = total[:SMALL // 2]
    vec1_ref[:] = total[SMALL // 2:]


def gather_head(*shards):
    part, model = shards[0].shape[2:]
    rows = 4 * part + SMALL
    vmem = pl.BlockSpec(memory_space=pltpu.VMEM)
    vec = sds((SMALL // 2, model), F32)
    mlp = sds((2 * GROUP, model), BF16)
    return pl.pallas_call(
        gather_kernel, in_specs=[vmem] * 7, out_specs=[vmem] * 6,
        out_shape=[sds((8, rows, model), BF16), vec, vec, sds((4 * part, model), BF16), mlp, mlp],
        scratch_shapes=[pltpu.VMEM((rows, model), BF16), pltpu.VMEM((SMALL, model), F32),
                        pltpu.SemaphoreType.DMA((14,)), pltpu.SemaphoreType.DMA((14,))],
        compiler_params=pltpu.CompilerParams(collective_id=0, has_side_effects=True, vmem_limit_bytes=VMEM_BYTES),
        cost_estimate=cost(1e9, 4e6), name='gather_head',
    )(*shards)


class Scatter:
    def __init__(self, src, own, out, bufs, sems, extra=()):
        rel = place()
        self.chunk = lambda r, c: rel(r // 2, r % 2, c)
        self.src, self.own, self.sems = src, own, sems
        self.targets = core, px, py = peers(rel)
        recv1, recv2, recv3, send2, send3, keep = bufs
        self.pieces = []
        for n, j in enumerate((0, 2, 1, 3)):
            self.pieces.append((src, own, out, j * PIECE, PIECE, j < 2, [b.at[n] for b in bufs]))
        for s, o, out_s, b in extra:
            self.pieces.append((s, o, out_s, 0, out_s.shape[0], True, b))
        self.first, self.second, self.third = [], [], []
        for n, (s, o, _, row, rows, x_first, b) in enumerate(self.pieces):
            self.first.append([remote(s.at[self.chunk(r, 1), pl.ds(row, rows)], b[0].at[r], sems[0:2], 4 * n + r, core)
                               for r in range(4)])
            self.second.append(remote(b[3], b[1], sems[2:4], n, px if x_first else py))
            self.third.append(remote(b[4], b[2], sems[4:6], n, py if x_first else px))
        self.local = [pltpu.make_async_copy(src.at[self.chunk(r, 0)], own.at[r], sems[6].at[r]) for r in range(4)]

    def stage_one(self):
        greet(self.targets)
        for copies in self.first:
            for copy in copies:
                copy.start()
        for copy in self.local:
            copy.start()

    def stage_two(self):
        for copy in self.local:
            copy.wait()
        for n, (_, o, _, row, rows, x_first, b) in enumerate(self.pieces):
            for copy in self.first[n]:
                copy.wait_recv()
            sent, kept = ((1, 3), (0, 2)) if x_first else ((2, 3), (0, 1))
            for i in range(2):
                b[3][i] = o[sent[i], row:row + rows, :] + b[0][sent[i]]
            for i in range(2):
                b[5][i] = o[kept[i], row:row + rows, :] + b[0][kept[i]]
            self.second[n].start()

    def stage_three(self):
        for n, (_, _, _, row, rows, _, b) in enumerate(self.pieces):
            self.second[n].wait_recv()
            b[4][:] = b[5][1] + b[1][1]
            b[5][0] = b[5][0] + b[1][0]
            self.third[n].start()

    def stage_four(self):
        for n, (_, _, out, row, rows, _, b) in enumerate(self.pieces):
            self.third[n].wait_recv()
            out[row:row + rows, :] = b[5][0] + b[2][:]
        for n, copies in enumerate(self.first):
            for copy in copies + [self.second[n], self.third[n]]:
                copy.wait_send()


def scatter_bufs(n, rows, model):
    lead = (n,) if n else ()
    shapes = [(4,), (2,), (), (2,), (), (2,)]
    return [pltpu.VMEM(lead + s + (rows, model), F32) for s in shapes]


def scatter_sems(n):
    dma = pltpu.SemaphoreType.DMA
    return [dma((4 * n,)), dma((4 * n,))] + [dma((n,))] * 4 + [dma((4,))]


def unpermute_lanes(x):
    half, wide = HEAD_DIM // 2, 2 * HEAD_DIM
    block = lax.broadcasted_iota(jnp.int32, (1, wide), 1) // half
    out = []
    for lo in range(0, x.shape[1], GROUP):
        pair = halves(x, lo)
        for j in range(2):
            acc = None
            for b in range(4):
                shift = half * (b - 2 * j - b // 2) % wide
                moved = pltpu.roll(pair[b % 2], shift, 1) if shift else pair[b % 2]
                acc = moved if acc is None else jnp.where(block == b, moved, acc)
            out.append(acc)
    return jnp.concatenate(out, axis=1)


def tail_kernel(ga_ref, sa1_ref, sa0_ref, sm1_ref, sm0_ref, out_ref, small_ref, own_ref, *rest):
    bufs, s_ref, so_ref, s_bufs, sems = rest[:6], rest[6], rest[7], rest[8:14], rest[14:]
    part = HEAD_DIM
    job = Scatter(ga_ref, own_ref, out_ref, bufs, sems, extra=[(s_ref, so_ref, small_ref, s_bufs)])
    s_ref[:] = jnp.zeros_like(s_ref)
    for l, (ga, gm) in enumerate(((sa0_ref, sm0_ref), (sa1_ref, sm1_ref))):
        base = l * SMALL // 2
        qk = unpermute_lanes(ga[:])
        for d in range(8):
            cols = slice(d * part, (d + 1) * part)
            s_ref[d, base:base + 2, :part] = qk[:2, cols]
            s_ref[d, base + 2:base + 6, :part] = ga[2:6, cols]
            s_ref[d, base + 6:base + 8, :part] = gm[5:7, cols]
            s_ref[d, base + 8:base + 9, :part] = gm[4:5, cols]
            for r in range(4):
                lo = d % 2 * GROUP + r * part
                s_ref[d, base + 9 + r:base + 10 + r, :part] = gm[d // 2:d // 2 + 1, lo:lo + part]
    for r in range(4):
        so_ref[pl.ds(r, 1)] = s_ref[pl.ds(job.chunk(r, 0), 1)]
    job.stage_one()
    job.stage_two()
    job.stage_three()
    job.stage_four()


def scatter_tail(g_a, *smalls):
    _, rows, model = g_a.shape
    wide = 2 * HEAD_DIM
    vmem = pl.BlockSpec(memory_space=pltpu.VMEM)
    n = rows // PIECE
    return pl.pallas_call(
        tail_kernel, in_specs=[pl.BlockSpec(memory_space=pl.ANY)] + [vmem] * 4, out_specs=[vmem] * 2,
        out_shape=[sds((rows, model), F32), sds((SMALL, wide), F32)],
        scratch_shapes=[pltpu.VMEM((4, rows, model), F32)] + scatter_bufs(n, PIECE, model)
        + [pltpu.VMEM((8, SMALL, wide), F32), pltpu.VMEM((4, SMALL, wide), F32)] + scatter_bufs(0, SMALL, wide)
        + scatter_sems(n + 1),
        compiler_params=pltpu.CompilerParams(collective_id=1, has_side_effects=True, vmem_limit_bytes=VMEM_BYTES),
        cost_estimate=cost(1e9, 8e6), name='scatter_tail',
    )(g_a, *smalls)


def finish_kernel(a0_ref, a1_ref, small_ref, m0_ref, m1_ref, ga_ref, gba_ref, gln_ref, gup_ref, gbu_ref, gdown_ref, gbd_ref):
    part, model = ga_ref.shape[2:]
    for l, (a_ref, m_ref) in enumerate(((a0_ref, m0_ref), (a1_ref, m1_ref))):
        for i in range(4):
            val = a_ref[i * part:(i + 1) * part, :]
            ga_ref[l, i] = unpermute_lanes(val) if i < 2 else val
            gup_ref[l, :, i * model:(i + 1) * model] = m_ref[i * part:(i + 1) * part, :]
        gdown_ref[l] = m_ref[4 * part:, :]
        base = l * SMALL // 2
        gba_ref[l] = small_ref[base:base + 4, :part]
        gln_ref[l] = small_ref[base + 4:base + 8, :part]
        gbd_ref[l:l + 1, :] = small_ref[base + 8:base + 9, :part]
        up = [small_ref[base + 9 + r:base + 10 + r, :part] for r in range(4)]
        gbu_ref[l:l + 1, :] = jnp.concatenate(up, axis=1)


def finish(shapes, *ins):
    vmem = pl.BlockSpec(memory_space=pltpu.VMEM)
    return pl.pallas_call(
        finish_kernel, in_specs=[vmem] * len(ins), out_specs=[vmem] * len(shapes), out_shape=shapes,
        compiler_params=pltpu.CompilerParams(vmem_limit_bytes=VMEM_BYTES), cost_estimate=cost(1e9, 6e6), name='finish',
    )(*ins)


def solution(mesh):
    axis = mesh.axis_names[0]
    batch_spec = P(axis)
    weight_specs = tuple(P(*([None] * k), axis) for k in (2, 2, 2, 1, 1, 1, 1))

    def gather(a):
        return lax.all_gather(a, axis, axis=0, tiled=False)

    def whole_step(x, lengths, d_y, *shards):
        model = x.shape[2]
        tables = rotary_tables(x.shape[1])
        tokens = (x.shape[0] * x.shape[1], model)
        head, vec0, vec1, attn_shard, mlp_shard0, mlp_shard1 = gather_head(*shards)
        vecs = (vec0, vec1)
        mlp_w0 = gather(mlp_shard0)
        attn_w = (head, gather(attn_shard))
        mlp_w = (mlp_w0, gather(mlp_shard1))

        hidden = x
        saved = []
        for l in range(2):
            *attn_saved, mid = attn_forward(lengths, hidden, attn_w[l], vecs[l], tables)
            mid2 = mid.reshape(tokens)
            y, act, slope = mlp_forward(mid2, mlp_w[l], vecs[l], FWD_ROWS)
            saved.append((hidden, attn_saved, mid2, act, slope))
            hidden = y.reshape(x.shape)

        grad = d_y.reshape(tokens)
        gw_attn, r_mlp, s_attn, s_mlp = None, {}, {}, {}
        for l in (1, 0):
            x_in, attn_saved, mid2, act, slope = saved[l]
            d_mid, gw_mlp, s_mlp[l], *done = mlp_backward(grad, mid2, act, slope, mlp_w[l], vecs[l], BWD_ROWS, gw_attn)
            r_mlp[l] = lax.psum_scatter(gw_mlp, axis, scatter_dimension=0, tiled=False)
            d_x, gw_attn, s_attn[l] = attn_backward(lengths, d_mid.reshape(x.shape), x_in, attn_saved, attn_w[l], vecs[l], tables)
            grad = d_x.reshape(tokens)
        a_sum0, small_sum = scatter_tail(gw_attn, s_attn[1], s_attn[0], s_mlp[1], s_mlp[0])
        shapes = [sds(s.shape, F32) for s in shards]
        outs = finish(shapes, a_sum0, *done, small_sum, r_mlp[0], r_mlp[1])
        return (d_x,) + tuple(outs)

    return jax.shard_map(whole_step, mesh=mesh,
                         in_specs=(batch_spec, batch_spec, batch_spec) + weight_specs,
                         out_specs=(batch_spec,) + weight_specs,
                         check_vma=False)
```

```python
import math
import numpy as np
import jax
import jax.numpy as jnp
from jax import lax
from jax.experimental import pallas as pl
from jax.experimental.pallas import tpu as pltpu
from jax.sharding import PartitionSpec as P

HEAD_DIM = 64
EPS = 1e-5
THETA = 10000.0
NEG_BIG = -1e30
BF16 = jnp.bfloat16
F32 = jnp.float32
VMEM_BYTES = 60 * 1024 * 1024
GROUP = 256
HEADS_GROUP = 4
KEY_BLOCK = 128
SEQS = 2
FWD_ROWS = 384
BWD_ROWS = (512, 768)

NN, NT, TN = (1, 0), (1, 1), (0, 0)


def mm(a, b, dims=NN):
    return lax.dot_general(a, b, (((dims[0],), (dims[1],)), ((), ())), preferred_element_type=F32)


def line(ref, i):
    return ref[i:i + 1, :]


def add_line(ref, i, block):
    ref[i:i + 1, :] += jnp.sum(block, axis=0, keepdims=True)


def row_mean(block):
    return jnp.mean(block, axis=-1, keepdims=True)


def row_sum(block):
    return jnp.sum(block, axis=-1, keepdims=True)


def square(w_ref, i):
    model = w_ref.shape[-1]
    return w_ref[:, i * HEAD_DIM:(i + 1) * HEAD_DIM, :].reshape(model, model)


def rotary_tables(seq_len):
    half_dim = HEAD_DIM // 2
    freq_pos = (np.arange(2 * HEAD_DIM) % half_dim).astype(np.float32)
    inv_freq = np.float32(1) / np.power(np.float32(THETA), freq_pos * np.float32(2 / HEAD_DIM))
    angles = np.arange(seq_len, dtype=np.float32)[:, None] * inv_freq[None, :]
    wide = angles.astype(np.float64)
    return jnp.asarray(np.cos(wide).astype(np.float32)), jnp.asarray(np.sin(wide).astype(np.float32))


def normalize(x_f32):
    centered = x_f32 - row_mean(x_f32)
    rstd = lax.rsqrt(row_mean(centered * centered) + EPS)
    return centered * rstd, rstd


def norm_bwd(d_h, x_hat, rstd, gain):
    d_hat = d_h * gain
    mean_d = row_mean(d_hat)
    mean_dx = row_mean(d_hat * x_hat)
    return rstd * (d_hat - mean_d - x_hat * mean_dx)


def halves(block, lo):
    mid = lo + GROUP // 2
    return block[:, lo:mid], block[:, mid:lo + GROUP]


def rot_halves(first, second, cos_tab, sin_tab):
    return first * cos_tab - second * sin_tab, second * cos_tab + first * sin_tab


def unrot_halves(first, second, cos_tab, sin_tab):
    return first * cos_tab + second * sin_tab, second * cos_tab - first * sin_tab


def head_masks():
    lane = lax.broadcasted_iota(jnp.int32, (1, GROUP), 1)
    qk = [((lane % 128) // 32 == h).astype(F32).astype(BF16) for h in range(HEADS_GROUP)]
    vo = [(lane // 64 == h).astype(F32).astype(BF16) for h in range(HEADS_GROUP)]
    return qk, vo


def stack_masked(block, masks):
    return jnp.concatenate([block * m for m in masks], axis=0)


def each_sequence(len_ref, seq_len, body):
    def one(i, carry):
        length = len_ref[pl.program_id(0) * SEQS + i]
        blocks = (length + KEY_BLOCK - 1) // KEY_BLOCK
        for n in range(1, seq_len // KEY_BLOCK + 1):
            @pl.when(blocks == n)
            def _(n=n):
                body(i, length, n * KEY_BLOCK)
        return carry

    lax.fori_loop(0, SEQS, one, 0)


def flat(ref):
    return ref[:].reshape(SEQS * ref.shape[1], ref.shape[2])


def repeat_rows(table):
    return jnp.concatenate([table[:]] * SEQS, axis=0)


def attn_fwd_kernel(len_ref, x_ref, w_ref, vec_ref, cos_ref, sin_ref, q_ref, k_ref, v_ref, p_ref, ctx_ref, mid_ref):
    seq_len, model = x_ref.shape[1:]
    x_hat, _ = normalize(flat(x_ref).astype(F32))
    h_one = (x_hat * line(vec_ref, 4) + line(vec_ref, 5)).astype(BF16)
    cos_tab, sin_tab = repeat_rows(cos_ref), repeat_rows(sin_ref)
    for i, out in enumerate((q_ref, k_ref)):
        proj = mm(h_one, square(w_ref, i)) + line(vec_ref, i)
        if i == 0:
            proj = proj * (HEAD_DIM ** -0.5)
        for g in range(model // GROUP):
            lo = g * GROUP
            first, second = rot_halves(*halves(proj, lo), cos_tab, sin_tab)
            turned = jnp.concatenate([first.astype(BF16), second.astype(BF16)], axis=1)
            out[:, :, lo:lo + GROUP] = turned.reshape(SEQS, seq_len, GROUP)
    proj = mm(h_one, square(w_ref, 2)) + line(vec_ref, 2)
    v_ref[:] = proj.astype(BF16).reshape(x_ref.shape)
    qk_masks, vo_masks = head_masks()

    def attend(b, length, width):
        valid = lax.broadcasted_iota(jnp.int32, (1, width), 1) < length
        for g in range(model // GROUP):
            lo = g * GROUP
            k_cat = stack_masked(k_ref[b, :width, lo:lo + GROUP], qk_masks)
            scores = mm(q_ref[b, :, lo:lo + GROUP], k_cat, NT)
            probs = []
            for h in range(HEADS_GROUP):
                s_h = jnp.where(valid, scores[:, h * width:(h + 1) * width], NEG_BIG)
                e_h = jnp.exp(s_h - jnp.max(s_h, axis=-1, keepdims=True))
                p_h = (e_h * (1.0 / row_sum(e_h))).astype(BF16)
                base = (g * HEADS_GROUP + h) * seq_len
                p_ref[b, :, base:base + width] = p_h
                probs.append(p_h)
            v_cat = stack_masked(v_ref[b, :width, lo:lo + GROUP], vo_masks)
            ctx_ref[b, :, lo:lo + GROUP] = mm(jnp.concatenate(probs, axis=1), v_cat).astype(BF16)

    each_sequence(len_ref, seq_len, attend)
    attn_out = mm(flat(ctx_ref), square(w_ref, 3))
    mid_ref[:] = (flat(x_ref).astype(F32) + attn_out + line(vec_ref, 3)).astype(BF16).reshape(x_ref.shape)


def gelu_parts(pre):
    cdf = 0.5 * lax.erf(pre * (1.0 / math.sqrt(2.0))) + 0.5
    density = jnp.exp(pre * pre * -0.5) * (1.0 / math.sqrt(2.0 * math.pi))
    return (pre * cdf).astype(BF16), cdf + pre * density


def mlp_fwd_kernel(mid_ref, w_ref, vec_ref, y_ref, act_ref, slope_ref):
    model = mid_ref.shape[1]
    mid = mid_ref[:].astype(F32)
    x_hat, _ = normalize(mid)
    h_two = (x_hat * line(vec_ref, 6) + line(vec_ref, 7)).astype(BF16)
    for c in range(4):
        cols = slice(c * model, (c + 1) * model)
        pre = mm(h_two, square(w_ref, c)) + line(vec_ref, 9 + c)
        act_ref[:, cols], slope_ref[:, cols] = gelu_parts(pre)
    out = mm(act_ref[:], w_ref[:, 256:512, :].reshape(4 * model, model))
    y_ref[:] = (mid + out + line(vec_ref, 8)).astype(BF16)


def mlp_bwd_scatter_kernel(dout_ref, mid_ref, act_ref, slope_ref, w_ref, vec_ref, ga_ref, dmid_ref, gw_ref, gs_ref, out_ref,
                           dpre_ref, own_ref, *rest):
    job = Scatter(ga_ref, own_ref, out_ref, rest[:6], rest[6:])
    step, last = pl.program_id(0), pl.num_programs(0) - 1
    pl.when(step == 0)(job.stage_one)
    pl.when(step == 1)(job.stage_two)
    pl.when(step == last - 1)(job.stage_three)
    mlp_bwd_kernel(dout_ref, mid_ref, act_ref, slope_ref, w_ref, vec_ref, dmid_ref, gw_ref, gs_ref, dpre_ref)
    pl.when(step == last)(job.stage_four)


def mlp_last_kernel(dout_ref, mid_ref, w_ref, vec_ref, dmid_ref, gw_ref, gs_ref, dpre_ref, act_ref):
    mlp_bwd_kernel(dout_ref, mid_ref, act_ref, None, w_ref, vec_ref, dmid_ref, gw_ref, gs_ref, dpre_ref)


def mlp_bwd_kernel(dout_ref, mid_ref, act_ref, slope_ref, w_ref, vec_ref, dmid_ref, gw_ref, gs_ref, dpre_ref):
    model = mid_ref.shape[1]

    @pl.when(pl.program_id(0) == 0)
    def _():
        gw_ref[:] = jnp.zeros_like(gw_ref)
        gs_ref[:] = jnp.zeros_like(gs_ref)

    x_hat, rstd = normalize(mid_ref[:].astype(F32))
    h_two = (x_hat * line(vec_ref, 6) + line(vec_ref, 7)).astype(BF16)
    d_out = dout_ref[:]
    d_h = None
    for c in range(4):
        cols = slice(c * model, (c + 1) * model)
        d_act = mm(d_out, w_ref[2 * c:2 * c + 2, 256:512, :].reshape(model, model), NT)
        if slope_ref is None:
            act_ref[:, cols], slope = gelu_parts(mm(h_two, square(w_ref, c)) + line(vec_ref, 9 + c))
        else:
            slope = slope_ref[:, cols]
        d_pre = d_act * slope
        add_line(gs_ref, c, d_pre)
        dpre_ref[:, cols] = d_pre.astype(BF16)
    for c in range(4):
        cols = slice(c * model, (c + 1) * model)
        gw_ref[2 * c:2 * c + 2, 256:512, :] += mm(act_ref[:, cols], d_out, TN).reshape(2, 256, model)
        gw_ref[:, c * 64:(c + 1) * 64, :] += mm(h_two, dpre_ref[:, cols], TN).reshape(8, 64, model)
        part = mm(dpre_ref[:, cols], square(w_ref, c), NT)
        d_h = part if d_h is None else d_h + part
    d_out_f32 = d_out.astype(F32)
    add_line(gs_ref, 4, d_out_f32)
    add_line(gs_ref, 5, d_h * x_hat)
    add_line(gs_ref, 6, d_h)
    dmid_ref[:] = (d_out_f32 + norm_bwd(d_h, x_hat, rstd, line(vec_ref, 6))).astype(BF16)


def attn_bwd_kernel(len_ref, dmid_ref, x_ref, q_ref, k_ref, v_ref, p_ref, ctx_ref, w_ref, vec_ref, cos_ref, sin_ref,
                    dx_ref, gw_ref, gs_ref, dctx_ref, dq_ref, dk_ref, dv_ref):
    seq_len, model = x_ref.shape[1:]

    @pl.when(pl.program_id(0) == 0)
    def _():
        gw_ref[:] = jnp.zeros_like(gw_ref)
        gs_ref[:] = jnp.zeros_like(gs_ref)

    d_mid = flat(dmid_ref)
    d_mid_f32 = d_mid.astype(F32)
    add_line(gs_ref, 3, d_mid_f32)
    gw_ref[:, 192:256, :] += mm(flat(ctx_ref), d_mid, TN).reshape(8, 64, model)
    dctx_ref[:] = mm(d_mid, square(w_ref, 3), NT).astype(BF16).reshape(x_ref.shape)
    qk_masks, vo_masks = head_masks()

    def attend(b, length, width):
        for g in range(model // GROUP):
            lo = g * GROUP
            d_ctx = dctx_ref[b, :, lo:lo + GROUP]
            d_probs = mm(d_ctx, stack_masked(v_ref[b, :width, lo:lo + GROUP], vo_masks), NT)
            ds_list, dst_list, pt_list = [], [], []
            for h in range(HEADS_GROUP):
                base = (g * HEADS_GROUP + h) * seq_len
                p_bf = p_ref[b, :, base:base + width]
                p_h = p_bf.astype(F32)
                dp_h = d_probs[:, h * width:(h + 1) * width]
                ds_h = (p_h * (dp_h - row_sum(dp_h * p_h))).astype(BF16)
                ds_list.append(ds_h)
                dst_list.append(ds_h.T)
                pt_list.append(p_bf.T)
            k_cat = stack_masked(k_ref[b, :width, lo:lo + GROUP], qk_masks)
            dq_ref[b, :, lo:lo + GROUP] = mm(jnp.concatenate(ds_list, axis=1), k_cat)
            q_cat = stack_masked(q_ref[b, :, lo:lo + GROUP], qk_masks)
            dk_ref[b, :width, lo:lo + GROUP] = mm(jnp.concatenate(dst_list, axis=1), q_cat)
            do_cat = stack_masked(d_ctx, vo_masks)
            dv_ref[b, :width, lo:lo + GROUP] = mm(jnp.concatenate(pt_list, axis=1), do_cat)
        if width < seq_len:
            dk_ref[b, width:, :] = jnp.zeros((seq_len - width, model), F32)
            dv_ref[b, width:, :] = jnp.zeros((seq_len - width, model), F32)

    each_sequence(len_ref, seq_len, attend)
    cos_tab, sin_tab = repeat_rows(cos_ref), repeat_rows(sin_ref)
    x_hat, rstd = normalize(flat(x_ref).astype(F32))
    h_one = (x_hat * line(vec_ref, 4) + line(vec_ref, 5)).astype(BF16)
    d_h = None
    for i, src in enumerate((dq_ref, dk_ref, dv_ref)):
        if i < 2:
            pieces = []
            for g in range(model // GROUP):
                lo = g * GROUP
                pieces.extend(unrot_halves(*halves(flat(src), lo), cos_tab, sin_tab))
            d_proj = jnp.concatenate(pieces, axis=1)
            if i == 0:
                d_proj = d_proj * (HEAD_DIM ** -0.5)
        else:
            d_proj = flat(src)
        d_proj = d_proj.astype(BF16)
        add_line(gs_ref, i, d_proj.astype(F32))
        gw_ref[:, i * 64:(i + 1) * 64, :] += mm(h_one, d_proj, TN).reshape(8, 64, model)
        part = mm(d_proj, square(w_ref, i), NT)
        d_h = part if d_h is None else d_h + part
    add_line(gs_ref, 4, d_h * x_hat)
    add_line(gs_ref, 5, d_h)
    dx_ref[:] = (d_mid_f32 + norm_bwd(d_h, x_hat, rstd, line(vec_ref, 4))).astype(BF16).reshape(x_ref.shape)


def seq_spec(*tail):
    return pl.BlockSpec((SEQS,) + tail, lambda b, *_: (b,) + (0,) * len(tail))


def row_spec(rows, cols):
    return pl.BlockSpec((rows, cols), lambda b, *_: (b, 0))


def whole(shape):
    return pl.BlockSpec(shape, lambda *_: (0,) * len(shape))


def params():
    return pltpu.CompilerParams(dimension_semantics=('arbitrary',), vmem_limit_bytes=VMEM_BYTES)


def cost(flops, nbytes):
    return pl.CostEstimate(flops=int(flops), bytes_accessed=int(nbytes), transcendentals=0)


def sds(shape, dtype):
    return jax.ShapeDtypeStruct(shape, dtype)


def attn_forward(lengths, x, w, vec, tables):
    n, seq_len, model = x.shape
    heads = model // HEAD_DIM
    act = sds(x.shape, BF16)
    spec = seq_spec(seq_len, model)
    return pl.pallas_call(
        attn_fwd_kernel,
        grid_spec=pltpu.PrefetchScalarGridSpec(
            num_scalar_prefetch=1, grid=(n // SEQS,),
            in_specs=[spec, whole((8, 256, model)), whole(vec.shape), whole(tables[0].shape), whole(tables[1].shape)],
            out_specs=[spec, spec, spec, seq_spec(seq_len, heads * seq_len), spec, spec]),
        out_shape=[act, act, act, sds((n, seq_len, heads * seq_len), BF16), act, act],
        compiler_params=params(), cost_estimate=cost(16e9, 40e6), name='attn_fwd',
    )(lengths, x, w, vec, *tables)


def mlp_forward(mid, w, vec, rows):
    tokens, model = mid.shape
    return pl.pallas_call(
        mlp_fwd_kernel, grid=(tokens // rows,),
        in_specs=[row_spec(rows, model), whole(w.shape), whole(vec.shape)],
        out_specs=[row_spec(rows, model), row_spec(rows, 4 * model), row_spec(rows, 4 * model)],
        out_shape=[sds(mid.shape, BF16), sds((tokens, 4 * model), BF16), sds((tokens, 4 * model), F32)],
        compiler_params=params(), cost_estimate=cost(13e9, 50e6), name='mlp_fwd',
    )(mid, w, vec)


def mlp_backward(d_out, mid, act, slope, w, vec, rows, g_a=None):
    tokens, model = mid.shape
    wide = row_spec(rows, 4 * model)
    in_specs = [row_spec(rows, model), row_spec(rows, model), wide, wide, whole(w.shape), whole(vec.shape)]
    out_specs = [row_spec(rows, model), whole(w.shape), whole((8, model))]
    out_shape = [sds(mid.shape, BF16), sds(w.shape, F32), sds((8, model), F32)]
    scratch = [pltpu.VMEM((rows, 4 * model), BF16)]
    ins, kernel, extra = (d_out, mid, act, slope, w, vec), mlp_bwd_kernel, {}
    if act is None:
        ins, kernel, in_specs = (d_out, mid, w, vec), mlp_last_kernel, in_specs[:2] + in_specs[4:]
        scratch = scratch + scratch
    if g_a is not None:
        ins, kernel, extra = ins + (g_a,), mlp_bwd_scatter_kernel, {'collective_id': 2, 'has_side_effects': True}
        in_specs.append(pl.BlockSpec(memory_space=pl.ANY))
        out_specs.append(whole(g_a.shape[1:]))
        out_shape.append(sds(g_a.shape[1:], F32))
        n = g_a.shape[1] // PIECE
        scratch += [pltpu.VMEM((4,) + g_a.shape[1:], F32)] + scatter_bufs(n, PIECE, model) + scatter_sems(n)
    return pl.pallas_call(
        kernel, grid=(tokens // rows,), in_specs=in_specs, out_specs=out_specs, out_shape=out_shape, scratch_shapes=scratch,
        compiler_params=pltpu.CompilerParams(dimension_semantics=('arbitrary',), vmem_limit_bytes=VMEM_BYTES, **extra),
        cost_estimate=cost(26e9, 60e6), name='mlp_bwd',
    )(*ins)


def attn_backward(lengths, d_mid, x, saved, w, vec, tables):
    n, seq_len, model = x.shape
    heads = model // HEAD_DIM
    spec = seq_spec(seq_len, model)
    return pl.pallas_call(
        attn_bwd_kernel,
        grid_spec=pltpu.PrefetchScalarGridSpec(
            num_scalar_prefetch=1, grid=(n // SEQS,),
            in_specs=[spec, spec, spec, spec, spec, seq_spec(seq_len, heads * seq_len), spec, whole((8, 256, model)),
                      whole(vec.shape), whole(tables[0].shape), whole(tables[1].shape)],
            out_specs=[spec, whole((8, 256, model)), whole((8, model))],
            scratch_shapes=[pltpu.VMEM((SEQS, seq_len, model), t) for t in (BF16, F32, F32, F32)]),
        out_shape=[sds(x.shape, BF16), sds((8, 256, model), F32), sds((8, model), F32)],
        compiler_params=params(), cost_estimate=cost(30e9, 50e6), name='attn_bwd',
    )(lengths, d_mid, x, *saved, w, vec, *tables)


MESH_ID = pl.DeviceIdType.MESH
PIECE = 64
SMALL = 32


def place():
    me = lax.axis_index('fsdp')
    core, x_bit, y_bit = lax.rem(me, 2), lax.rem(me // 2, 2), me // 4

    def rel(ry, rx, rc):
        return lax.rem(y_bit + ry, 2) * 4 + lax.rem(x_bit + rx, 2) * 2 + lax.rem(core + rc, 2)

    return rel


def peers(rel):
    return rel(0, 0, 1), rel(0, 1, 0), rel(1, 0, 0)


def greet(targets):
    barrier = pltpu.get_barrier_semaphore()
    for peer in targets:
        pl.semaphore_signal(barrier, device_id=(peer,), device_id_type=MESH_ID)
    pl.semaphore_wait(barrier, len(targets))


def remote(src, dst, sems, i, peer):
    return pltpu.make_async_remote_copy(src_ref=src, dst_ref=dst, send_sem=sems[0].at[i], recv_sem=sems[1].at[i],
                                        device_id=(peer,), device_id_type=MESH_ID)


def pack_small(dst, me, perm, b_attn, ln_par, b_up, b_down):
    part, model = b_attn.shape[-1], dst.shape[-1]
    spot = (lax.broadcasted_iota(jnp.int32, (part, model), 1) == lax.broadcasted_iota(jnp.int32, (part, model), 0) + me * part)
    spot = spot.astype(F32).astype(BF16)
    lane = lax.broadcasted_iota(jnp.int32, (4, model), 1)
    row = lax.broadcasted_iota(jnp.int32, (4, model), 0)
    here = (row == me // 2) & (lane // GROUP == lax.rem(me, 2))
    dst[:] = jnp.zeros_like(dst)
    for l in range(b_attn.shape[0]):
        base = l * SMALL // 2
        bias = mm(b_attn[l], spot)
        dst[base:base + 2, :] = permute_mm(bias[:2].astype(BF16), perm)
        dst[base + 2:base + 4, :] = bias[2:]
        dst[base + 4:base + 8, :] = mm(ln_par[l], spot)
        dst[base + 8:base + 9, :] = mm(b_down[l:l + 1, :], spot)
        up = b_up[l:l + 1, :].astype(F32)
        dst[base + 9:base + 13, :] = jnp.where(here, jnp.concatenate([up, up], axis=1), 0.0)


def permutation():
    old = lax.broadcasted_iota(jnp.int32, (GROUP, GROUP), 0)
    new = lax.broadcasted_iota(jnp.int32, (GROUP, GROUP), 1)
    half = HEAD_DIM // 2
    want = (new % 128) // half * HEAD_DIM + new // 128 * half + new % half
    return (old == want).astype(F32).astype(BF16)


def permute_mm(block, perm):
    return jnp.concatenate([mm(block[:, lo:lo + GROUP], perm) for lo in range(0, block.shape[1], GROUP)], axis=1)


def pack_attn(write, w_layer, perm):
    part = w_layer.shape[1]
    for i in range(4):
        rows = w_layer[i]
        write(slice(i * part, (i + 1) * part), permute_mm(rows, perm).astype(BF16) if i < 2 else rows)


def gather_kernel(w_attn, b_attn, ln_par, w_up, b_up, w_down, b_down, out_ref, vec0_ref, vec1_ref, attn_ref, mlp0_ref, mlp1_ref,
                  pack_ref, small_ref, send_sem, recv_sem):
    rel = place()
    core, px, py = peers(rel)
    me, diag = rel(0, 0, 0), rel(1, 1, 0)
    part, model = w_attn.shape[2:]
    perm = permutation()

    def put(rows, value):
        pack_ref[rows, :] = value

    def put_second(rows, value):
        attn_ref[rows, :] = value

    pack_small(small_ref, me, perm, b_attn, ln_par, b_up, b_down)
    pack_ref[4 * part:, :] = small_ref[:].astype(BF16)
    pack_attn(put, w_attn[0], perm)
    rows = pack_ref.shape[0]
    top, low = pl.ds(0, rows // 2), pl.ds(rows // 2, rows // 2)
    sems = (send_sem, recv_sem)
    greet((core, px, py))

    ids = iter(range(send_sem.shape[0]))

    def own(rows, peer):
        return remote(pack_ref.at[rows], out_ref.at[me, rows], sems, next(ids), peer)

    def pass_on(slot, rows, peer):
        return remote(out_ref.at[slot, rows], out_ref.at[slot, rows], sems, next(ids), peer)

    x_late, x_soon = own(top, px), own(low, px)
    y_soon, y_late = own(top, py), own(low, py)
    c_one, c_two = own(top, core), own(low, core)
    for copy in (x_soon, y_soon, x_late, y_late, c_one, c_two):
        copy.start()
    out_ref[pl.ds(me, 1)] = pack_ref[:][None]
    on_x, on_y = pass_on(py, top, px), pass_on(px, low, py)
    steps = [(y_soon, on_x, pass_on(py, top, core)), (x_soon, on_y, pass_on(px, low, core)),
             (x_late, None, pass_on(px, top, core)), (y_late, None, pass_on(py, low, core)),
             (on_x, None, pass_on(diag, top, core)), (on_y, None, pass_on(diag, low, core))]
    for arrived, onward, across in steps:
        arrived.wait_recv()
        if onward:
            onward.start()
        across.start()
    pack_attn(put_second, w_attn[1], perm)
    for l, mlp_ref in enumerate((mlp0_ref, mlp1_ref)):
        for c in range(4):
            mlp_ref[c * part:(c + 1) * part, :] = w_up[l, :, c * model:(c + 1) * model]
        mlp_ref[4 * part:, :] = w_down[l]
    from_core = [c_one, c_two] + [across for _, _, across in steps]
    for copy in from_core:
        copy.wait_recv()
    for copy in from_core + [arrived for arrived, _, _ in steps]:
        copy.wait_send()
    total = sum(out_ref[d, 4 * part:, :].astype(F32) for d in range(8))
    vec0_ref[:] = total[:SMALL // 2]
    vec1_ref[:] = total[SMALL // 2:]


def gather_head(*shards):
    part, model = shards[0].shape[2:]
    rows = 4 * part + SMALL
    vmem = pl.BlockSpec(memory_space=pltpu.VMEM)
    vec = sds((SMALL // 2, model), F32)
    mlp = sds((2 * GROUP, model), BF16)
    return pl.pallas_call(
        gather_kernel, in_specs=[vmem] * 7, out_specs=[vmem] * 6,
        out_shape=[sds((8, rows, model), BF16), vec, vec, sds((4 * part, model), BF16), mlp, mlp],
        scratch_shapes=[pltpu.VMEM((rows, model), BF16), pltpu.VMEM((SMALL, model), F32),
                        pltpu.SemaphoreType.DMA((14,)), pltpu.SemaphoreType.DMA((14,))],
        compiler_params=pltpu.CompilerParams(collective_id=0, has_side_effects=True, vmem_limit_bytes=VMEM_BYTES),
        cost_estimate=cost(1e9, 4e6), name='gather_head',
    )(*shards)


class Scatter:
    def __init__(self, src, own, out, bufs, sems, extra=()):
        rel = place()
        self.chunk = lambda r, c: rel(r // 2, r % 2, c)
        self.src, self.own, self.sems = src, own, sems
        self.targets = core, px, py = peers(rel)
        recv1, recv2, recv3, send2, send3, keep = bufs
        self.pieces = []
        for n, j in enumerate((0, 2, 1, 3)):
            self.pieces.append((src, own, out, j * PIECE, PIECE, j < 2, [b.at[n] for b in bufs]))
        for s, o, out_s, b in extra:
            self.pieces.append((s, o, out_s, 0, out_s.shape[0], True, b))
        self.first, self.second, self.third = [], [], []
        for n, (s, o, _, row, rows, x_first, b) in enumerate(self.pieces):
            self.first.append([remote(s.at[self.chunk(r, 1), pl.ds(row, rows)], b[0].at[r], sems[0:2], 4 * n + r, core)
                               for r in range(4)])
            self.second.append(remote(b[3], b[1], sems[2:4], n, px if x_first else py))
            self.third.append(remote(b[4], b[2], sems[4:6], n, py if x_first else px))
        self.local = [pltpu.make_async_copy(src.at[self.chunk(r, 0)], own.at[r], sems[6].at[r]) for r in range(4)]

    def stage_one(self):
        greet(self.targets)
        for copies in self.first:
            for copy in copies:
                copy.start()
        for copy in self.local:
            copy.start()

    def stage_two(self):
        for copy in self.local:
            copy.wait()
        for n, (_, o, _, row, rows, x_first, b) in enumerate(self.pieces):
            for copy in self.first[n]:
                copy.wait_recv()
            sent, kept = ((1, 3), (0, 2)) if x_first else ((2, 3), (0, 1))
            for i in range(2):
                b[3][i] = o[sent[i], row:row + rows, :] + b[0][sent[i]]
            for i in range(2):
                b[5][i] = o[kept[i], row:row + rows, :] + b[0][kept[i]]
            self.second[n].start()

    def stage_three(self):
        for n, (_, _, _, row, rows, _, b) in enumerate(self.pieces):
            self.second[n].wait_recv()
            b[4][:] = b[5][1] + b[1][1]
            b[5][0] = b[5][0] + b[1][0]
            self.third[n].start()

    def stage_four(self):
        for n, (_, _, out, row, rows, _, b) in enumerate(self.pieces):
            self.third[n].wait_recv()
            out[row:row + rows, :] = b[5][0] + b[2][:]
        for n, copies in enumerate(self.first):
            for copy in copies + [self.second[n], self.third[n]]:
                copy.wait_send()


def scatter_bufs(n, rows, model):
    lead = (n,) if n else ()
    shapes = [(4,), (2,), (), (2,), (), (2,)]
    return [pltpu.VMEM(lead + s + (rows, model), F32) for s in shapes]


def scatter_sems(n):
    dma = pltpu.SemaphoreType.DMA
    return [dma((4 * n,)), dma((4 * n,))] + [dma((n,))] * 4 + [dma((4,))]


def unpermute_lanes(x):
    half, wide = HEAD_DIM // 2, 2 * HEAD_DIM
    block = lax.broadcasted_iota(jnp.int32, (1, wide), 1) // half
    out = []
    for lo in range(0, x.shape[1], GROUP):
        pair = halves(x, lo)
        for j in range(2):
            acc = None
            for b in range(4):
                shift = half * (b - 2 * j - b // 2) % wide
                moved = pltpu.roll(pair[b % 2], shift, 1) if shift else pair[b % 2]
                acc = moved if acc is None else jnp.where(block == b, moved, acc)
            out.append(acc)
    return jnp.concatenate(out, axis=1)


def tail_kernel(ga_ref, sa1_ref, sa0_ref, sm1_ref, sm0_ref, out_ref, small_ref, own_ref, *rest):
    bufs, s_ref, so_ref, s_bufs, sems = rest[:6], rest[6], rest[7], rest[8:14], rest[14:]
    part = HEAD_DIM
    job = Scatter(ga_ref, own_ref, out_ref, bufs, sems, extra=[(s_ref, so_ref, small_ref, s_bufs)])
    s_ref[:] = jnp.zeros_like(s_ref)
    for l, (ga, gm) in enumerate(((sa0_ref, sm0_ref), (sa1_ref, sm1_ref))):
        base = l * SMALL // 2
        qk = unpermute_lanes(ga[:])
        for d in range(8):
            cols = slice(d * part, (d + 1) * part)
            s_ref[d, base:base + 2, :part] = qk[:2, cols]
            s_ref[d, base + 2:base + 6, :part] = ga[2:6, cols]
            s_ref[d, base + 6:base + 8, :part] = gm[5:7, cols]
            s_ref[d, base + 8:base + 9, :part] = gm[4:5, cols]
            for r in range(4):
                lo = d % 2 * GROUP + r * part
                s_ref[d, base + 9 + r:base + 10 + r, :part] = gm[d // 2:d // 2 + 1, lo:lo + part]
    for r in range(4):
        so_ref[pl.ds(r, 1)] = s_ref[pl.ds(job.chunk(r, 0), 1)]
    job.stage_one()
    job.stage_two()
    job.stage_three()
    job.stage_four()


def scatter_tail(g_a, *smalls):
    _, rows, model = g_a.shape
    wide = 2 * HEAD_DIM
    vmem = pl.BlockSpec(memory_space=pltpu.VMEM)
    n = rows // PIECE
    return pl.pallas_call(
        tail_kernel, in_specs=[pl.BlockSpec(memory_space=pl.ANY)] + [vmem] * 4, out_specs=[vmem] * 2,
        out_shape=[sds((rows, model), F32), sds((SMALL, wide), F32)],
        scratch_shapes=[pltpu.VMEM((4, rows, model), F32)] + scatter_bufs(n, PIECE, model)
        + [pltpu.VMEM((8, SMALL, wide), F32), pltpu.VMEM((4, SMALL, wide), F32)] + scatter_bufs(0, SMALL, wide)
        + scatter_sems(n + 1),
        compiler_params=pltpu.CompilerParams(collective_id=1, has_side_effects=True, vmem_limit_bytes=VMEM_BYTES),
        cost_estimate=cost(1e9, 8e6), name='scatter_tail',
    )(g_a, *smalls)


def finish_kernel(a0_ref, a1_ref, small_ref, m0_ref, m1_ref, ga_ref, gba_ref, gln_ref, gup_ref, gbu_ref, gdown_ref, gbd_ref):
    part, model = ga_ref.shape[2:]
    for l, (a_ref, m_ref) in enumerate(((a0_ref, m0_ref), (a1_ref, m1_ref))):
        for i in range(4):
            val = a_ref[i * part:(i + 1) * part, :]
            ga_ref[l, i] = unpermute_lanes(val) if i < 2 else val
            gup_ref[l, :, i * model:(i + 1) * model] = m_ref[i * part:(i + 1) * part, :]
        gdown_ref[l] = m_ref[4 * part:, :]
        base = l * SMALL // 2
        gba_ref[l] = small_ref[base:base + 4, :part]
        gln_ref[l] = small_ref[base + 4:base + 8, :part]
        gbd_ref[l:l + 1, :] = small_ref[base + 8:base + 9, :part]
        up = [small_ref[base + 9 + r:base + 10 + r, :part] for r in range(4)]
        gbu_ref[l:l + 1, :] = jnp.concatenate(up, axis=1)


def finish(shapes, *ins):
    vmem = pl.BlockSpec(memory_space=pltpu.VMEM)
    return pl.pallas_call(
        finish_kernel, in_specs=[vmem] * len(ins), out_specs=[vmem] * len(shapes), out_shape=shapes,
        compiler_params=pltpu.CompilerParams(vmem_limit_bytes=VMEM_BYTES), cost_estimate=cost(1e9, 6e6), name='finish',
    )(*ins)


def solution(mesh):
    axis = mesh.axis_names[0]
    batch_spec = P(axis)
    weight_specs = tuple(P(*([None] * k), axis) for k in (2, 2, 2, 1, 1, 1, 1))

    def gather(a):
        return lax.all_gather(a, axis, axis=0, tiled=False)

    def whole_step(x, lengths, d_y, *shards):
        model = x.shape[2]
        tables = rotary_tables(x.shape[1])
        tokens = (x.shape[0] * x.shape[1], model)
        head, vec0, vec1, attn_shard, mlp_shard0, mlp_shard1 = gather_head(*shards)
        vecs = (vec0, vec1)
        mlp_w0 = gather(mlp_shard0)
        attn_w = (head, gather(attn_shard))
        mlp_w = (mlp_w0, gather(mlp_shard1))

        hidden = x
        saved = []
        for l in range(2):
            *attn_saved, mid = attn_forward(lengths, hidden, attn_w[l], vecs[l], tables)
            mid2 = mid.reshape(tokens)
            act = slope = None
            if l == 0:
                y, act, slope = mlp_forward(mid2, mlp_w[l], vecs[l], FWD_ROWS)
            saved.append((hidden, attn_saved, mid2, act, slope))
            hidden = y.reshape(x.shape)

        grad = d_y.reshape(tokens)
        gw_attn, r_mlp, s_attn, s_mlp = None, {}, {}, {}
        for l in (1, 0):
            x_in, attn_saved, mid2, act, slope = saved[l]
            d_mid, gw_mlp, s_mlp[l], *done = mlp_backward(grad, mid2, act, slope, mlp_w[l], vecs[l], BWD_ROWS[l], gw_attn)
            r_mlp[l] = lax.psum_scatter(gw_mlp, axis, scatter_dimension=0, tiled=False)
            d_x, gw_attn, s_attn[l] = attn_backward(lengths, d_mid.reshape(x.shape), x_in, attn_saved, attn_w[l], vecs[l], tables)
            grad = d_x.reshape(tokens)
        a_sum0, small_sum = scatter_tail(gw_attn, s_attn[1], s_attn[0], s_mlp[1], s_mlp[0])
        shapes = [sds(s.shape, F32) for s in shards]
        outs = finish(shapes, a_sum0, *done, small_sum, r_mlp[0], r_mlp[1])
        return (d_x,) + tuple(outs)

    return jax.shard_map(whole_step, mesh=mesh,
                         in_specs=(batch_spec, batch_spec, batch_spec) + weight_specs,
                         out_specs=(batch_spec,) + weight_specs,
                         check_vma=False)
```

```python
import math
import numpy as np
import jax
import jax.numpy as jnp
from jax import lax
from jax.experimental import pallas as pl
from jax.experimental.pallas import tpu as pltpu
from jax.sharding import PartitionSpec as P

HEAD_DIM = 64
EPS = 1e-5
THETA = 10000.0
NEG_BIG = -1e30
BF16 = jnp.bfloat16
F32 = jnp.float32
VMEM_BYTES = 60 * 1024 * 1024
GROUP = 256
HEADS_GROUP = 4
KEY_BLOCK = 128
SEQS = 2
FWD_ROWS = 384
BWD_ROWS = (512, 768)

NN, NT, TN = (1, 0), (1, 1), (0, 0)


def mm(a, b, dims=NN):
    return lax.dot_general(a, b, (((dims[0],), (dims[1],)), ((), ())), preferred_element_type=F32)


def line(ref, i):
    return ref[i:i + 1, :]


def add_line(ref, i, block):
    ref[i:i + 1, :] += jnp.sum(block, axis=0, keepdims=True)


def row_mean(block):
    return jnp.mean(block, axis=-1, keepdims=True)


def row_sum(block):
    return jnp.sum(block, axis=-1, keepdims=True)


def square(w_ref, i):
    model = w_ref.shape[-1]
    return w_ref[:, i * HEAD_DIM:(i + 1) * HEAD_DIM, :].reshape(model, model)


def rotary_tables(seq_len):
    half_dim = HEAD_DIM // 2
    freq_pos = (np.arange(2 * HEAD_DIM) % half_dim).astype(np.float32)
    inv_freq = np.float32(1) / np.power(np.float32(THETA), freq_pos * np.float32(2 / HEAD_DIM))
    angles = np.arange(seq_len, dtype=np.float32)[:, None] * inv_freq[None, :]
    wide = angles.astype(np.float64)
    return jnp.asarray(np.cos(wide).astype(np.float32)), jnp.asarray(np.sin(wide).astype(np.float32))


def normalize(x_f32):
    centered = x_f32 - row_mean(x_f32)
    rstd = lax.rsqrt(row_mean(centered * centered) + EPS)
    return centered * rstd, rstd


def norm_bwd(d_h, x_hat, rstd, gain):
    d_hat = d_h * gain
    mean_d = row_mean(d_hat)
    mean_dx = row_mean(d_hat * x_hat)
    return rstd * (d_hat - mean_d - x_hat * mean_dx)


def halves(block, lo):
    mid = lo + GROUP // 2
    return block[:, lo:mid], block[:, mid:lo + GROUP]


def rot_halves(first, second, cos_tab, sin_tab):
    return first * cos_tab - second * sin_tab, second * cos_tab + first * sin_tab


def unrot_halves(first, second, cos_tab, sin_tab):
    return first * cos_tab + second * sin_tab, second * cos_tab - first * sin_tab


def head_masks():
    lane = lax.broadcasted_iota(jnp.int32, (1, GROUP), 1)
    qk = [((lane % 128) // 32 == h).astype(F32).astype(BF16) for h in range(HEADS_GROUP)]
    vo = [(lane // 64 == h).astype(F32).astype(BF16) for h in range(HEADS_GROUP)]
    return qk, vo


def stack_masked(block, masks):
    return jnp.concatenate([block * m for m in masks], axis=0)


def each_sequence(len_ref, seq_len, body):
    def one(i, carry):
        length = len_ref[pl.program_id(0) * SEQS + i]
        blocks = (length + KEY_BLOCK - 1) // KEY_BLOCK
        for n in range(1, seq_len // KEY_BLOCK + 1):
            @pl.when(blocks == n)
            def _(n=n):
                body(i, length, n * KEY_BLOCK)
        return carry

    lax.fori_loop(0, SEQS, one, 0)


def flat(ref):
    return ref[:].reshape(SEQS * ref.shape[1], ref.shape[2])


def repeat_rows(table):
    return jnp.concatenate([table[:]] * SEQS, axis=0)


def attn_fwd_kernel(len_ref, x_ref, w_ref, vec_ref, cos_ref, sin_ref, q_ref, k_ref, v_ref, p_ref, ctx_ref, mid_ref):
    seq_len, model = x_ref.shape[1:]
    x_hat, _ = normalize(flat(x_ref).astype(F32))
    h_one = (x_hat * line(vec_ref, 4) + line(vec_ref, 5)).astype(BF16)
    cos_tab, sin_tab = repeat_rows(cos_ref), repeat_rows(sin_ref)
    for i, out in enumerate((q_ref, k_ref)):
        proj = mm(h_one, square(w_ref, i)) + line(vec_ref, i)
        if i == 0:
            proj = proj * (HEAD_DIM ** -0.5)
        for g in range(model // GROUP):
            lo = g * GROUP
            first, second = rot_halves(*halves(proj, lo), cos_tab, sin_tab)
            turned = jnp.concatenate([first.astype(BF16), second.astype(BF16)], axis=1)
            out[:, :, lo:lo + GROUP] = turned.reshape(SEQS, seq_len, GROUP)
    proj = mm(h_one, square(w_ref, 2)) + line(vec_ref, 2)
    v_ref[:] = proj.astype(BF16).reshape(x_ref.shape)
    qk_masks, vo_masks = head_masks()

    def attend(b, length, width):
        open_keys = width - KEY_BLOCK
        valid = lax.broadcasted_iota(jnp.int32, (1, KEY_BLOCK), 1) < length - open_keys
        all_scores = []
        for lo in range(0, model, GROUP):
            k_cat = stack_masked(k_ref[b, :width, lo:lo + GROUP], qk_masks)
            all_scores.append(mm(q_ref[b, :, lo:lo + GROUP], k_cat, NT))
        for g, scores in enumerate(all_scores):
            lo = g * GROUP
            probs = []
            for h in range(HEADS_GROUP):
                s_h = scores[:, h * width:(h + 1) * width]
                last = jnp.where(valid, s_h[:, open_keys:], NEG_BIG)
                s_h = jnp.concatenate([s_h[:, :open_keys], last], axis=1) if open_keys else last
                e_h = jnp.exp(s_h - jnp.max(s_h, axis=-1, keepdims=True))
                p_h = (e_h * (1.0 / row_sum(e_h))).astype(BF16)
                base = (g * HEADS_GROUP + h) * seq_len
                p_ref[b, :, base:base + width] = p_h
                probs.append(p_h)
            v_cat = stack_masked(v_ref[b, :width, lo:lo + GROUP], vo_masks)
            ctx_ref[b, :, lo:lo + GROUP] = mm(jnp.concatenate(probs, axis=1), v_cat).astype(BF16)

    each_sequence(len_ref, seq_len, attend)
    attn_out = mm(flat(ctx_ref), square(w_ref, 3))
    mid_ref[:] = (flat(x_ref).astype(F32) + attn_out + line(vec_ref, 3)).astype(BF16).reshape(x_ref.shape)


def gelu_parts(pre):
    cdf = 0.5 * lax.erf(pre * (1.0 / math.sqrt(2.0))) + 0.5
    density = jnp.exp(pre * pre * -0.5) * (1.0 / math.sqrt(2.0 * math.pi))
    return (pre * cdf).astype(BF16), cdf + pre * density


def mlp_fwd_kernel(mid_ref, w_ref, vec_ref, y_ref, act_ref, slope_ref):
    model = mid_ref.shape[1]
    mid = mid_ref[:].astype(F32)
    x_hat, _ = normalize(mid)
    h_two = (x_hat * line(vec_ref, 6) + line(vec_ref, 7)).astype(BF16)
    for c in range(4):
        cols = slice(c * model, (c + 1) * model)
        pre = mm(h_two, square(w_ref, c)) + line(vec_ref, 9 + c)
        act_ref[:, cols], slope_ref[:, cols] = gelu_parts(pre)
    out = mm(act_ref[:], w_ref[:, 256:512, :].reshape(4 * model, model))
    y_ref[:] = (mid + out + line(vec_ref, 8)).astype(BF16)


def mlp_bwd_scatter_kernel(dout_ref, mid_ref, act_ref, slope_ref, w_ref, vec_ref, ga_ref, dmid_ref, gw_ref, gs_ref, out_ref,
                           dpre_ref, own_ref, *rest):
    job = Scatter(ga_ref, own_ref, out_ref, rest[:6], rest[6:])
    step, last = pl.program_id(0), pl.num_programs(0) - 1
    pl.when(step == 0)(job.stage_one)
    pl.when(step == 1)(job.stage_two)
    pl.when(step == last - 1)(job.stage_three)
    mlp_bwd_kernel(dout_ref, mid_ref, act_ref, slope_ref, w_ref, vec_ref, dmid_ref, gw_ref, gs_ref, dpre_ref)
    pl.when(step == last)(job.stage_four)


def mlp_last_kernel(dout_ref, mid_ref, w_ref, vec_ref, dmid_ref, gw_ref, gs_ref, dpre_ref, act_ref):
    mlp_bwd_kernel(dout_ref, mid_ref, act_ref, None, w_ref, vec_ref, dmid_ref, gw_ref, gs_ref, dpre_ref)


def mlp_bwd_kernel(dout_ref, mid_ref, act_ref, slope_ref, w_ref, vec_ref, dmid_ref, gw_ref, gs_ref, dpre_ref):
    model = mid_ref.shape[1]

    @pl.when(pl.program_id(0) == 0)
    def _():
        gw_ref[:] = jnp.zeros_like(gw_ref)
        gs_ref[:] = jnp.zeros_like(gs_ref)

    x_hat, rstd = normalize(mid_ref[:].astype(F32))
    h_two = (x_hat * line(vec_ref, 6) + line(vec_ref, 7)).astype(BF16)
    d_out = dout_ref[:]
    d_h = None
    for c in range(4):
        cols = slice(c * model, (c + 1) * model)
        d_act = mm(d_out, w_ref[2 * c:2 * c + 2, 256:512, :].reshape(model, model), NT)
        if slope_ref is None:
            act_ref[:, cols], slope = gelu_parts(mm(h_two, square(w_ref, c)) + line(vec_ref, 9 + c))
        else:
            slope = slope_ref[:, cols]
        d_pre = d_act * slope
        add_line(gs_ref, c, d_pre)
        dpre_ref[:, cols] = d_pre.astype(BF16)
    for c in range(4):
        cols = slice(c * model, (c + 1) * model)
        gw_ref[2 * c:2 * c + 2, 256:512, :] += mm(act_ref[:, cols], d_out, TN).reshape(2, 256, model)
        gw_ref[:, c * 64:(c + 1) * 64, :] += mm(h_two, dpre_ref[:, cols], TN).reshape(8, 64, model)
        part = mm(dpre_ref[:, cols], square(w_ref, c), NT)
        d_h = part if d_h is None else d_h + part
    d_out_f32 = d_out.astype(F32)
    add_line(gs_ref, 4, d_out_f32)
    add_line(gs_ref, 5, d_h * x_hat)
    add_line(gs_ref, 6, d_h)
    dmid_ref[:] = (d_out_f32 + norm_bwd(d_h, x_hat, rstd, line(vec_ref, 6))).astype(BF16)


def attn_bwd_kernel(len_ref, dmid_ref, x_ref, q_ref, k_ref, v_ref, p_ref, ctx_ref, w_ref, vec_ref, cos_ref, sin_ref,
                    dx_ref, gw_ref, gs_ref, dctx_ref, dq_ref, dk_ref, dv_ref):
    seq_len, model = x_ref.shape[1:]

    @pl.when(pl.program_id(0) == 0)
    def _():
        gw_ref[:] = jnp.zeros_like(gw_ref)
        gs_ref[:] = jnp.zeros_like(gs_ref)

    d_mid = flat(dmid_ref)
    d_mid_f32 = d_mid.astype(F32)
    add_line(gs_ref, 3, d_mid_f32)
    gw_ref[:, 192:256, :] += mm(flat(ctx_ref), d_mid, TN).reshape(8, 64, model)
    dctx_ref[:] = mm(d_mid, square(w_ref, 3), NT).astype(BF16).reshape(x_ref.shape)
    qk_masks, vo_masks = head_masks()

    def attend(b, length, width):
        all_dp = []
        for lo in range(0, model, GROUP):
            all_dp.append(mm(dctx_ref[b, :, lo:lo + GROUP], stack_masked(v_ref[b, :width, lo:lo + GROUP], vo_masks), NT))
        for g, d_probs in enumerate(all_dp):
            lo = g * GROUP
            d_ctx = dctx_ref[b, :, lo:lo + GROUP]
            ds_list, dst_list, pt_list = [], [], []
            for h in range(HEADS_GROUP):
                base = (g * HEADS_GROUP + h) * seq_len
                p_bf = p_ref[b, :, base:base + width]
                p_h = p_bf.astype(F32)
                dp_h = d_probs[:, h * width:(h + 1) * width]
                ds_h = (p_h * (dp_h - row_sum(dp_h * p_h))).astype(BF16)
                ds_list.append(ds_h)
                dst_list.append(ds_h.T)
                pt_list.append(p_bf.T)
            k_cat = stack_masked(k_ref[b, :width, lo:lo + GROUP], qk_masks)
            dq_ref[b, :, lo:lo + GROUP] = mm(jnp.concatenate(ds_list, axis=1), k_cat)
            q_cat = stack_masked(q_ref[b, :, lo:lo + GROUP], qk_masks)
            dk_ref[b, :width, lo:lo + GROUP] = mm(jnp.concatenate(dst_list, axis=1), q_cat)
            do_cat = stack_masked(d_ctx, vo_masks)
            dv_ref[b, :width, lo:lo + GROUP] = mm(jnp.concatenate(pt_list, axis=1), do_cat)
        if width < seq_len:
            dk_ref[b, width:, :] = jnp.zeros((seq_len - width, model), F32)
            dv_ref[b, width:, :] = jnp.zeros((seq_len - width, model), F32)

    each_sequence(len_ref, seq_len, attend)
    cos_tab, sin_tab = repeat_rows(cos_ref), repeat_rows(sin_ref)
    x_hat, rstd = normalize(flat(x_ref).astype(F32))
    h_one = (x_hat * line(vec_ref, 4) + line(vec_ref, 5)).astype(BF16)
    d_h = None
    for i, src in enumerate((dq_ref, dk_ref, dv_ref)):
        if i < 2:
            pieces = []
            for g in range(model // GROUP):
                lo = g * GROUP
                pieces.extend(unrot_halves(*halves(flat(src), lo), cos_tab, sin_tab))
            d_proj = jnp.concatenate(pieces, axis=1)
            if i == 0:
                d_proj = d_proj * (HEAD_DIM ** -0.5)
        else:
            d_proj = flat(src)
        d_proj = d_proj.astype(BF16)
        add_line(gs_ref, i, d_proj.astype(F32))
        gw_ref[:, i * 64:(i + 1) * 64, :] += mm(h_one, d_proj, TN).reshape(8, 64, model)
        part = mm(d_proj, square(w_ref, i), NT)
        d_h = part if d_h is None else d_h + part
    add_line(gs_ref, 4, d_h * x_hat)
    add_line(gs_ref, 5, d_h)
    dx_ref[:] = (d_mid_f32 + norm_bwd(d_h, x_hat, rstd, line(vec_ref, 4))).astype(BF16).reshape(x_ref.shape)


def seq_spec(*tail):
    return pl.BlockSpec((SEQS,) + tail, lambda b, *_: (b,) + (0,) * len(tail))


def row_spec(rows, cols):
    return pl.BlockSpec((rows, cols), lambda b, *_: (b, 0))


def whole(shape):
    return pl.BlockSpec(shape, lambda *_: (0,) * len(shape))


def params():
    return pltpu.CompilerParams(dimension_semantics=('arbitrary',), vmem_limit_bytes=VMEM_BYTES)


def cost(flops, nbytes):
    return pl.CostEstimate(flops=int(flops), bytes_accessed=int(nbytes), transcendentals=0)


def sds(shape, dtype):
    return jax.ShapeDtypeStruct(shape, dtype)


def attn_forward(lengths, x, w, vec, tables):
    n, seq_len, model = x.shape
    heads = model // HEAD_DIM
    act = sds(x.shape, BF16)
    spec = seq_spec(seq_len, model)
    return pl.pallas_call(
        attn_fwd_kernel,
        grid_spec=pltpu.PrefetchScalarGridSpec(
            num_scalar_prefetch=1, grid=(n // SEQS,),
            in_specs=[spec, whole((8, 256, model)), whole(vec.shape), whole(tables[0].shape), whole(tables[1].shape)],
            out_specs=[spec, spec, spec, seq_spec(seq_len, heads * seq_len), spec, spec]),
        out_shape=[act, act, act, sds((n, seq_len, heads * seq_len), BF16), act, act],
        compiler_params=params(), cost_estimate=cost(16e9, 40e6), name='attn_fwd',
    )(lengths, x, w, vec, *tables)


def mlp_forward(mid, w, vec, rows):
    tokens, model = mid.shape
    return pl.pallas_call(
        mlp_fwd_kernel, grid=(tokens // rows,),
        in_specs=[row_spec(rows, model), whole(w.shape), whole(vec.shape)],
        out_specs=[row_spec(rows, model), row_spec(rows, 4 * model), row_spec(rows, 4 * model)],
        out_shape=[sds(mid.shape, BF16), sds((tokens, 4 * model), BF16), sds((tokens, 4 * model), F32)],
        compiler_params=params(), cost_estimate=cost(13e9, 50e6), name='mlp_fwd',
    )(mid, w, vec)


def mlp_backward(d_out, mid, act, slope, w, vec, rows, g_a=None):
    tokens, model = mid.shape
    wide = row_spec(rows, 4 * model)
    in_specs = [row_spec(rows, model), row_spec(rows, model), wide, wide, whole(w.shape), whole(vec.shape)]
    out_specs = [row_spec(rows, model), whole(w.shape), whole((8, model))]
    out_shape = [sds(mid.shape, BF16), sds(w.shape, F32), sds((8, model), F32)]
    scratch = [pltpu.VMEM((rows, 4 * model), BF16)]
    ins, kernel, extra = (d_out, mid, act, slope, w, vec), mlp_bwd_kernel, {}
    if act is None:
        ins, kernel, in_specs = (d_out, mid, w, vec), mlp_last_kernel, in_specs[:2] + in_specs[4:]
        scratch = scratch + scratch
    if g_a is not None:
        ins, kernel, extra = ins + (g_a,), mlp_bwd_scatter_kernel, {'collective_id': 2, 'has_side_effects': True}
        in_specs.append(pl.BlockSpec(memory_space=pl.ANY))
        out_specs.append(whole(g_a.shape[1:]))
        out_shape.append(sds(g_a.shape[1:], F32))
        n = g_a.shape[1] // PIECE
        scratch += [pltpu.VMEM((4,) + g_a.shape[1:], F32)] + scatter_bufs(n, PIECE, model) + scatter_sems(n)
    return pl.pallas_call(
        kernel, grid=(tokens // rows,), in_specs=in_specs, out_specs=out_specs, out_shape=out_shape, scratch_shapes=scratch,
        compiler_params=pltpu.CompilerParams(dimension_semantics=('arbitrary',), vmem_limit_bytes=VMEM_BYTES, **extra),
        cost_estimate=cost(26e9, 60e6), name='mlp_bwd',
    )(*ins)


def attn_backward(lengths, d_mid, x, saved, w, vec, tables):
    n, seq_len, model = x.shape
    heads = model // HEAD_DIM
    spec = seq_spec(seq_len, model)
    return pl.pallas_call(
        attn_bwd_kernel,
        grid_spec=pltpu.PrefetchScalarGridSpec(
            num_scalar_prefetch=1, grid=(n // SEQS,),
            in_specs=[spec, spec, spec, spec, spec, seq_spec(seq_len, heads * seq_len), spec, whole((8, 256, model)),
                      whole(vec.shape), whole(tables[0].shape), whole(tables[1].shape)],
            out_specs=[spec, whole((8, 256, model)), whole((8, model))],
            scratch_shapes=[pltpu.VMEM((SEQS, seq_len, model), t) for t in (BF16, F32, F32, F32)]),
        out_shape=[sds(x.shape, BF16), sds((8, 256, model), F32), sds((8, model), F32)],
        compiler_params=params(), cost_estimate=cost(30e9, 50e6), name='attn_bwd',
    )(lengths, d_mid, x, *saved, w, vec, *tables)


MESH_ID = pl.DeviceIdType.MESH
PIECE = 64
SMALL = 32


def place():
    me = lax.axis_index('fsdp')
    core, x_bit, y_bit = lax.rem(me, 2), lax.rem(me // 2, 2), me // 4

    def rel(ry, rx, rc):
        return lax.rem(y_bit + ry, 2) * 4 + lax.rem(x_bit + rx, 2) * 2 + lax.rem(core + rc, 2)

    return rel


def peers(rel):
    return rel(0, 0, 1), rel(0, 1, 0), rel(1, 0, 0)


def greet(targets):
    barrier = pltpu.get_barrier_semaphore()
    for peer in targets:
        pl.semaphore_signal(barrier, device_id=(peer,), device_id_type=MESH_ID)
    pl.semaphore_wait(barrier, len(targets))


def remote(src, dst, sems, i, peer):
    return pltpu.make_async_remote_copy(src_ref=src, dst_ref=dst, send_sem=sems[0].at[i], recv_sem=sems[1].at[i],
                                        device_id=(peer,), device_id_type=MESH_ID)


def pack_small(dst, me, perm, b_attn, ln_par, b_up, b_down):
    part, model = b_attn.shape[-1], dst.shape[-1]
    spot = (lax.broadcasted_iota(jnp.int32, (part, model), 1) == lax.broadcasted_iota(jnp.int32, (part, model), 0) + me * part)
    spot = spot.astype(F32).astype(BF16)
    lane = lax.broadcasted_iota(jnp.int32, (4, model), 1)
    row = lax.broadcasted_iota(jnp.int32, (4, model), 0)
    here = (row == me // 2) & (lane // GROUP == lax.rem(me, 2))
    dst[:] = jnp.zeros_like(dst)
    for l in range(b_attn.shape[0]):
        base = l * SMALL // 2
        bias = mm(b_attn[l], spot)
        dst[base:base + 2, :] = permute_mm(bias[:2].astype(BF16), perm)
        dst[base + 2:base + 4, :] = bias[2:]
        dst[base + 4:base + 8, :] = mm(ln_par[l], spot)
        dst[base + 8:base + 9, :] = mm(b_down[l:l + 1, :], spot)
        up = b_up[l:l + 1, :].astype(F32)
        dst[base + 9:base + 13, :] = jnp.where(here, jnp.concatenate([up, up], axis=1), 0.0)


def permutation():
    old = lax.broadcasted_iota(jnp.int32, (GROUP, GROUP), 0)
    new = lax.broadcasted_iota(jnp.int32, (GROUP, GROUP), 1)
    half = HEAD_DIM // 2
    want = (new % 128) // half * HEAD_DIM + new // 128 * half + new % half
    return (old == want).astype(F32).astype(BF16)


def permute_mm(block, perm):
    return jnp.concatenate([mm(block[:, lo:lo + GROUP], perm) for lo in range(0, block.shape[1], GROUP)], axis=1)


def pack_attn(write, w_layer, perm):
    part = w_layer.shape[1]
    for i in range(4):
        rows = w_layer[i]
        write(slice(i * part, (i + 1) * part), permute_mm(rows, perm).astype(BF16) if i < 2 else rows)


def gather_kernel(w_attn, b_attn, ln_par, w_up, b_up, w_down, b_down, out_ref, vec0_ref, vec1_ref, attn_ref, mlp0_ref, mlp1_ref,
                  pack_ref, small_ref, send_sem, recv_sem):
    rel = place()
    core, px, py = peers(rel)
    me, diag = rel(0, 0, 0), rel(1, 1, 0)
    part, model = w_attn.shape[2:]
    perm = permutation()

    def put(rows, value):
        pack_ref[rows, :] = value

    def put_second(rows, value):
        attn_ref[rows, :] = value

    pack_small(small_ref, me, perm, b_attn, ln_par, b_up, b_down)
    pack_ref[4 * part:, :] = small_ref[:].astype(BF16)
    pack_attn(put, w_attn[0], perm)
    rows = pack_ref.shape[0]
    top, low = pl.ds(0, rows // 2), pl.ds(rows // 2, rows // 2)
    sems = (send_sem, recv_sem)
    greet((core, px, py))

    ids = iter(range(send_sem.shape[0]))

    def own(rows, peer):
        return remote(pack_ref.at[rows], out_ref.at[me, rows], sems, next(ids), peer)

    def pass_on(slot, rows, peer):
        return remote(out_ref.at[slot, rows], out_ref.at[slot, rows], sems, next(ids), peer)

    x_late, x_soon = own(top, px), own(low, px)
    y_soon, y_late = own(top, py), own(low, py)
    c_one, c_two = own(top, core), own(low, core)
    for copy in (x_soon, y_soon, x_late, y_late, c_one, c_two):
        copy.start()
    out_ref[pl.ds(me, 1)] = pack_ref[:][None]
    on_x, on_y = pass_on(py, top, px), pass_on(px, low, py)
    steps = [(y_soon, on_x, pass_on(py, top, core)), (x_soon, on_y, pass_on(px, low, core)),
             (x_late, None, pass_on(px, top, core)), (y_late, None, pass_on(py, low, core)),
             (on_x, None, pass_on(diag, top, core)), (on_y, None, pass_on(diag, low, core))]
    for arrived, onward, across in steps:
        arrived.wait_recv()
        if onward:
            onward.start()
        across.start()
    pack_attn(put_second, w_attn[1], perm)
    for l, mlp_ref in enumerate((mlp0_ref, mlp1_ref)):
        for c in range(4):
            mlp_ref[c * part:(c + 1) * part, :] = w_up[l, :, c * model:(c + 1) * model]
        mlp_ref[4 * part:, :] = w_down[l]
    from_core = [c_one, c_two] + [across for _, _, across in steps]
    for copy in from_core:
        copy.wait_recv()
    for copy in from_core + [arrived for arrived, _, _ in steps]:
        copy.wait_send()
    total = sum(out_ref[d, 4 * part:, :].astype(F32) for d in range(8))
    vec0_ref[:] = total[:SMALL // 2]
    vec1_ref[:] = total[SMALL // 2:]


def gather_head(*shards):
    part, model = shards[0].shape[2:]
    rows = 4 * part + SMALL
    vmem = pl.BlockSpec(memory_space=pltpu.VMEM)
    vec = sds((SMALL // 2, model), F32)
    mlp = sds((2 * GROUP, model), BF16)
    return pl.pallas_call(
        gather_kernel, in_specs=[vmem] * 7, out_specs=[vmem] * 6,
        out_shape=[sds((8, rows, model), BF16), vec, vec, sds((4 * part, model), BF16), mlp, mlp],
        scratch_shapes=[pltpu.VMEM((rows, model), BF16), pltpu.VMEM((SMALL, model), F32),
                        pltpu.SemaphoreType.DMA((14,)), pltpu.SemaphoreType.DMA((14,))],
        compiler_params=pltpu.CompilerParams(collective_id=0, has_side_effects=True, vmem_limit_bytes=VMEM_BYTES),
        cost_estimate=cost(1e9, 4e6), name='gather_head',
    )(*shards)


class Scatter:
    def __init__(self, src, own, out, bufs, sems, extra=()):
        rel = place()
        self.chunk = lambda r, c: rel(r // 2, r % 2, c)
        self.src, self.own, self.sems = src, own, sems
        self.targets = core, px, py = peers(rel)
        recv1, recv2, recv3, send2, send3, keep = bufs
        self.pieces = []
        for n, j in enumerate((0, 2, 1, 3)):
            self.pieces.append((src, own, out, j * PIECE, PIECE, j < 2, [b.at[n] for b in bufs]))
        for s, o, out_s, b in extra:
            self.pieces.append((s, o, out_s, 0, out_s.shape[0], True, b))
        self.first, self.second, self.third = [], [], []
        for n, (s, o, _, row, rows, x_first, b) in enumerate(self.pieces):
            self.first.append([remote(s.at[self.chunk(r, 1), pl.ds(row, rows)], b[0].at[r], sems[0:2], 4 * n + r, core)
                               for r in range(4)])
            self.second.append(remote(b[3], b[1], sems[2:4], n, px if x_first else py))
            self.third.append(remote(b[4], b[2], sems[4:6], n, py if x_first else px))
        self.local = [pltpu.make_async_copy(src.at[self.chunk(r, 0)], own.at[r], sems[6].at[r]) for r in range(4)]

    def stage_one(self):
        greet(self.targets)
        for copies in self.first:
            for copy in copies:
                copy.start()
        for copy in self.local:
            copy.start()

    def stage_two(self):
        for copy in self.local:
            copy.wait()
        for n, (_, o, _, row, rows, x_first, b) in enumerate(self.pieces):
            for copy in self.first[n]:
                copy.wait_recv()
            sent, kept = ((1, 3), (0, 2)) if x_first else ((2, 3), (0, 1))
            for i in range(2):
                b[3][i] = o[sent[i], row:row + rows, :] + b[0][sent[i]]
            for i in range(2):
                b[5][i] = o[kept[i], row:row + rows, :] + b[0][kept[i]]
            self.second[n].start()

    def stage_three(self):
        for n, (_, _, _, row, rows, _, b) in enumerate(self.pieces):
            self.second[n].wait_recv()
            b[4][:] = b[5][1] + b[1][1]
            b[5][0] = b[5][0] + b[1][0]
            self.third[n].start()

    def stage_four(self):
        for n, (_, _, out, row, rows, _, b) in enumerate(self.pieces):
            self.third[n].wait_recv()
            out[row:row + rows, :] = b[5][0] + b[2][:]
        for n, copies in enumerate(self.first):
            for copy in copies + [self.second[n], self.third[n]]:
                copy.wait_send()


def scatter_bufs(n, rows, model):
    lead = (n,) if n else ()
    shapes = [(4,), (2,), (), (2,), (), (2,)]
    return [pltpu.VMEM(lead + s + (rows, model), F32) for s in shapes]


def scatter_sems(n):
    dma = pltpu.SemaphoreType.DMA
    return [dma((4 * n,)), dma((4 * n,))] + [dma((n,))] * 4 + [dma((4,))]


def unpermute_lanes(x):
    half, wide = HEAD_DIM // 2, 2 * HEAD_DIM
    block = lax.broadcasted_iota(jnp.int32, (1, wide), 1) // half
    out = []
    for lo in range(0, x.shape[1], GROUP):
        pair = halves(x, lo)
        for j in range(2):
            acc = None
            for b in range(4):
                shift = half * (b - 2 * j - b // 2) % wide
                moved = pltpu.roll(pair[b % 2], shift, 1) if shift else pair[b % 2]
                acc = moved if acc is None else jnp.where(block == b, moved, acc)
            out.append(acc)
    return jnp.concatenate(out, axis=1)


def tail_kernel(ga_ref, sa1_ref, sa0_ref, sm1_ref, sm0_ref, out_ref, small_ref, own_ref, *rest):
    bufs, s_ref, so_ref, s_bufs, sems = rest[:6], rest[6], rest[7], rest[8:14], rest[14:]
    part = HEAD_DIM
    job = Scatter(ga_ref, own_ref, out_ref, bufs, sems, extra=[(s_ref, so_ref, small_ref, s_bufs)])
    s_ref[:] = jnp.zeros_like(s_ref)
    for l, (ga, gm) in enumerate(((sa0_ref, sm0_ref), (sa1_ref, sm1_ref))):
        base = l * SMALL // 2
        qk = unpermute_lanes(ga[:])
        for d in range(8):
            cols = slice(d * part, (d + 1) * part)
            s_ref[d, base:base + 2, :part] = qk[:2, cols]
            s_ref[d, base + 2:base + 6, :part] = ga[2:6, cols]
            s_ref[d, base + 6:base + 8, :part] = gm[5:7, cols]
            s_ref[d, base + 8:base + 9, :part] = gm[4:5, cols]
            for r in range(4):
                lo = d % 2 * GROUP + r * part
                s_ref[d, base + 9 + r:base + 10 + r, :part] = gm[d // 2:d // 2 + 1, lo:lo + part]
    for r in range(4):
        so_ref[pl.ds(r, 1)] = s_ref[pl.ds(job.chunk(r, 0), 1)]
    job.stage_one()
    job.stage_two()
    job.stage_three()
    job.stage_four()


def scatter_tail(g_a, *smalls):
    _, rows, model = g_a.shape
    wide = 2 * HEAD_DIM
    vmem = pl.BlockSpec(memory_space=pltpu.VMEM)
    n = rows // PIECE
    return pl.pallas_call(
        tail_kernel, in_specs=[pl.BlockSpec(memory_space=pl.ANY)] + [vmem] * 4, out_specs=[vmem] * 2,
        out_shape=[sds((rows, model), F32), sds((SMALL, wide), F32)],
        scratch_shapes=[pltpu.VMEM((4, rows, model), F32)] + scatter_bufs(n, PIECE, model)
        + [pltpu.VMEM((8, SMALL, wide), F32), pltpu.VMEM((4, SMALL, wide), F32)] + scatter_bufs(0, SMALL, wide)
        + scatter_sems(n + 1),
        compiler_params=pltpu.CompilerParams(collective_id=1, has_side_effects=True, vmem_limit_bytes=VMEM_BYTES),
        cost_estimate=cost(1e9, 8e6), name='scatter_tail',
    )(g_a, *smalls)


def finish_kernel(a0_ref, a1_ref, small_ref, m0_ref, m1_ref, ga_ref, gba_ref, gln_ref, gup_ref, gbu_ref, gdown_ref, gbd_ref):
    part, model = ga_ref.shape[2:]
    for l, (a_ref, m_ref) in enumerate(((a0_ref, m0_ref), (a1_ref, m1_ref))):
        for i in range(4):
            val = a_ref[i * part:(i + 1) * part, :]
            ga_ref[l, i] = unpermute_lanes(val) if i < 2 else val
            gup_ref[l, :, i * model:(i + 1) * model] = m_ref[i * part:(i + 1) * part, :]
        gdown_ref[l] = m_ref[4 * part:, :]
        base = l * SMALL // 2
        gba_ref[l] = small_ref[base:base + 4, :part]
        gln_ref[l] = small_ref[base + 4:base + 8, :part]
        gbd_ref[l:l + 1, :] = small_ref[base + 8:base + 9, :part]
        up = [small_ref[base + 9 + r:base + 10 + r, :part] for r in range(4)]
        gbu_ref[l:l + 1, :] = jnp.concatenate(up, axis=1)


def finish(shapes, *ins):
    vmem = pl.BlockSpec(memory_space=pltpu.VMEM)
    return pl.pallas_call(
        finish_kernel, in_specs=[vmem] * len(ins), out_specs=[vmem] * len(shapes), out_shape=shapes,
        compiler_params=pltpu.CompilerParams(vmem_limit_bytes=VMEM_BYTES), cost_estimate=cost(1e9, 6e6), name='finish',
    )(*ins)


def solution(mesh):
    axis = mesh.axis_names[0]
    batch_spec = P(axis)
    weight_specs = tuple(P(*([None] * k), axis) for k in (2, 2, 2, 1, 1, 1, 1))

    def gather(a):
        return lax.all_gather(a, axis, axis=0, tiled=False)

    def whole_step(x, lengths, d_y, *shards):
        model = x.shape[2]
        tables = rotary_tables(x.shape[1])
        tokens = (x.shape[0] * x.shape[1], model)
        head, vec0, vec1, attn_shard, mlp_shard0, mlp_shard1 = gather_head(*shards)
        vecs = (vec0, vec1)
        mlp_w0 = gather(mlp_shard0)
        attn_w = (head, gather(attn_shard))
        mlp_w = (mlp_w0, gather(mlp_shard1))

        hidden = x
        saved = []
        for l in range(2):
            *attn_saved, mid = attn_forward(lengths, hidden, attn_w[l], vecs[l], tables)
            mid2 = mid.reshape(tokens)
            act = slope = None
            if l == 0:
                y, act, slope = mlp_forward(mid2, mlp_w[l], vecs[l], FWD_ROWS)
            saved.append((hidden, attn_saved, mid2, act, slope))
            hidden = y.reshape(x.shape)

        grad = d_y.reshape(tokens)
        gw_attn, r_mlp, s_attn, s_mlp = None, {}, {}, {}
        for l in (1, 0):
            x_in, attn_saved, mid2, act, slope = saved[l]
            d_mid, gw_mlp, s_mlp[l], *done = mlp_backward(grad, mid2, act, slope, mlp_w[l], vecs[l], BWD_ROWS[l], gw_attn)
            r_mlp[l] = lax.psum_scatter(gw_mlp, axis, scatter_dimension=0, tiled=False)
            d_x, gw_attn, s_attn[l] = attn_backward(lengths, d_mid.reshape(x.shape), x_in, attn_saved, attn_w[l], vecs[l], tables)
            grad = d_x.reshape(tokens)
        a_sum0, small_sum = scatter_tail(gw_attn, s_attn[1], s_attn[0], s_mlp[1], s_mlp[0])
        shapes = [sds(s.shape, F32) for s in shards]
        outs = finish(shapes, a_sum0, *done, small_sum, r_mlp[0], r_mlp[1])
        return (d_x,) + tuple(outs)

    return jax.shard_map(whole_step, mesh=mesh,
                         in_specs=(batch_spec, batch_spec, batch_spec) + weight_specs,
                         out_specs=(batch_spec,) + weight_specs,
                         check_vma=False)
```
